32 devices in a mesh: groups: 2 (over y), gx: 4 (over z), gy: 4 (over x, core).
Axes of the slice: x: 2, y: 2, z: 4, core: 2. Of those that a mesh axis runs over, the one named last changes fastest.
Arguments:
- tokens: bfloat16 [2, 16, 16384], P(None, 'groups', 'gx'), parts along dimension 1, may hold values from -20 to 20, as said below
- lengths: int32 [2, 16], P(None, ('groups', 'gx')), parts along dimension 1, may hold values from 1 to 1024, as said below
- norm_gain: bfloat16 [16384], P('gx'), may hold values from 0.5 to 2
- w_query: bfloat16 [16384, 8192], P('gx', 'gy'), may hold values from -1.171875 to 1.171875
- key_value_weight: bfloat16 [16384, 4, 256], P('gx', 'gy'), may hold values from -0.046875 to 0.046875
- w_out: bfloat16 [8192, 16384], P('gy', 'gx'), may hold values from -0.0625 to 0.0625
- cache: bfloat16 [2, 16, 1024, 4, 2, 128], P(None, ('groups', 'gx'), None, 'gy'), parts along dimension 1, may hold values from -16 to 16
Outputs:
- layer_out: bfloat16 [2, 16, 16384], P(None, 'groups', 'gx'), parts along dimension 1
The draws below stay inside these ranges and needn't reach their ends.
There are 2 independent parts, one for each index of `groups`. The reference program is written for one: setup_inputs(seed, part) draws one part's arguments, and reference() takes and returns one part's arrays. A program takes and returns all parts, laid end to end along the dimension named above; an argument that names none is the same for every part. Nothing has to cross between parts.
Inputs may be any that keep to these rules, and one draw needn't show every extreme that they name: `tokens`: entries vary with the feature and the row. `lengths`: some rollout has exactly 1024 cached positions in every draw.
All inputs are finite; a program needn't handle non-finite values.
Results may differ from the reference program's by a relative error of at most 0.012.
The reference program's roundings to bfloat16 on the way count: a program that leaves them out, or rounds other values in their place, can miss the bound.
Values may be sent and summed in bfloat16 or wider, within the bound.
No kernel may reach another device: no remote copies, remote signals or barrier semaphores. Data moves between devices by JAX's collectives and lax.ppermute only.
A program may use at most 128 MiB of HBM per device.

```python
import math
import jax
import jax.numpy as jnp
from jax import lax

MODEL_WIDTH = 16384
QUERY_HEADS = 64
KEY_VALUE_HEADS = 4
HEAD_SIZE = 128
MICRO_BATCHES = 2
CACHE_POSITIONS = 1024
BATCH_ROLLOUTS = 8


def draw_tokens(key, part):
    first = jax.random.fold_in(key, 0)
    columns = jnp.exp(jnp.linspace(jnp.log(0.5), jnp.log(1.5), MODEL_WIDTH)).astype(jnp.float32)
    base = jax.random.truncated_normal(first, -6.0, 6.0, (MICRO_BATCHES, BATCH_ROLLOUTS, MODEL_WIDTH), jnp.float32)
    return (base * columns).astype(jnp.bfloat16)


def draw_lengths(key, part):
    counts = jax.random.randint(key, (MICRO_BATCHES, BATCH_ROLLOUTS), 1, CACHE_POSITIONS + 1, dtype=jnp.int32)
    return counts.at[0, 0].set(CACHE_POSITIONS)


def draw_w_query(key, part):
    first = jax.random.fold_in(jax.random.fold_in(key, 7), 0)
    base = jax.random.truncated_normal(first, -6.0, 6.0, (MODEL_WIDTH, QUERY_HEADS * HEAD_SIZE), jnp.float32) * MODEL_WIDTH ** (-0.5)
    return base.astype(jnp.bfloat16)


def draw_cache(key, part):
    factor = jnp.array([2.5, 1.0], dtype=jnp.float32).reshape(1, 1, 1, 1, 2, 1)
    array_shape = (MICRO_BATCHES, BATCH_ROLLOUTS, CACHE_POSITIONS, KEY_VALUE_HEADS, 2, HEAD_SIZE)
    base = jax.random.truncated_normal(key, -6.0, 6.0, array_shape, jnp.float32)
    return (base * factor).astype(jnp.bfloat16)


def block_levels(key, extent, cuts, low, largest):
    gain, own = 1.0, jax.random.fold_in(key, 6)
    for dim, shards_of in cuts:
        draws = jnp.exp(jax.random.uniform(jax.random.fold_in(own, dim), (shards_of,), jnp.float32, low / len(cuts), largest / len(cuts)))
        gain = gain * jnp.repeat(draws, extent[dim] // shards_of).reshape([-1 if axis == dim else 1 for axis in range(len(extent))])
    return gain


def scatter_about(own_key, shape, width, reach, cuts=(), held_as=jnp.bfloat16):
    drawn = jax.random.normal(own_key, shape, jnp.float32) * width
    if len(cuts) > 0:
        drawn = block_levels(own_key, shape, cuts, -0.22, 0.18) * drawn
    return jnp.clip(drawn, min=-reach, max=reach).astype(held_as)


def setup_inputs(seed: int = 0, part: int = 0) -> dict:
    arg_keys = jax.random.split(jax.random.key(seed), 8)
    own_keys = jax.random.split(jax.random.fold_in(arg_keys[7], part), 8)
    return {
        "tokens": draw_tokens(jax.random.fold_in(jax.random.fold_in(arg_keys[7], part), 71), part),
        "lengths": draw_lengths(jax.random.fold_in(jax.random.fold_in(arg_keys[7], part), 71), part),
        "norm_gain": jnp.clip(jnp.exp(math.log(2.0) - 1.3862944 * jax.random.uniform(arg_keys[2], (MODEL_WIDTH,), jnp.float32) ** block_levels(arg_keys[2], (MODEL_WIDTH,), ((0, 4),), -0.2, 0.2)), 0.5, 2.0).astype(jnp.bfloat16),
        "w_query": draw_w_query(jax.random.fold_in(arg_keys[7], 71), part),
        "key_value_weight": scatter_about(arg_keys[4], (MODEL_WIDTH, KEY_VALUE_HEADS, 2 * HEAD_SIZE), MODEL_WIDTH ** -0.5, 0.046875, ((0, 4), (1, 4))),
        "w_out": scatter_about(arg_keys[5], (QUERY_HEADS * HEAD_SIZE, MODEL_WIDTH), (QUERY_HEADS * HEAD_SIZE) ** -0.5, 0.0625, ((0, 4), (1, 4))),
        "cache": draw_cache(jax.random.fold_in(jax.random.fold_in(arg_keys[7], part), 71), part),
    }


def rotate(vectors, positions):
    half = vectors.shape[-1] // 2
    freq = 500000.0 ** (-2.0 * jnp.arange(half, dtype=jnp.float32) / vectors.shape[-1])
    angle = positions[..., None] * freq
    cosine = jnp.cos(angle)
    sine = jnp.sin(angle)
    first = vectors[..., :half]
    second = vectors[..., half:]
    return jnp.concatenate([first * cosine - second * sine, second * cosine + first * sine], axis=-1)

def reference(tokens, lengths, norm_gain, w_query, key_value_weight, w_out, cache):
    x_full = tokens.astype(jnp.float32)
    score_scale = lax.rsqrt(lax.optimization_barrier(jnp.mean(x_full * x_full, axis=-1)) + 1e-05)
    normed = (x_full * norm_gain.astype(jnp.float32)).astype(jnp.bfloat16)
    flattened = normed.reshape(MICRO_BATCHES * BATCH_ROLLOUTS, MODEL_WIDTH)
    query = jnp.dot(flattened, w_query, preferred_element_type=jnp.float32).reshape(MICRO_BATCHES, BATCH_ROLLOUTS, QUERY_HEADS, HEAD_SIZE)
    query = query * score_scale[:, :, None, None]
    key_value = jnp.dot(flattened, key_value_weight.reshape(MODEL_WIDTH, KEY_VALUE_HEADS * 2 * HEAD_SIZE), preferred_element_type=jnp.float32)
    key_value = key_value.reshape(MICRO_BATCHES, BATCH_ROLLOUTS, KEY_VALUE_HEADS, 2 * HEAD_SIZE) * score_scale[:, :, None, None]
    positions = lengths.astype(jnp.float32)[:, :, None]
    rotated_query = rotate(query, positions).astype(jnp.bfloat16)
    rkey = rotate(key_value[..., :HEAD_SIZE], positions)
    value_new = key_value[..., HEAD_SIZE:]
    query_group = QUERY_HEADS // KEY_VALUE_HEADS
    group_queries = rotated_query.reshape(MICRO_BATCHES, BATCH_ROLLOUTS, KEY_VALUE_HEADS, query_group, HEAD_SIZE)
    inv_root = 1.0 / jnp.sqrt(jnp.float32(HEAD_SIZE))

    def one_batch(items):
        qpart, kpart, vpart, cpart, lpart = items
        keys = cpart[:, :, :, 0, :].astype(jnp.float32)
        values = cpart[:, :, :, 1, :].astype(jnp.float32)
        qfull = qpart.astype(jnp.float32)
        scores = jnp.einsum('rkgd,rskd->rkgs', qfull, keys, precision=lax.Precision.HIGHEST) * inv_root
        valid = jnp.arange(CACHE_POSITIONS, dtype=jnp.int32)[None, :] < lpart[:, None]
        scores = jnp.where(valid[:, None, None, :], scores, -1e+30)
        new_score = lax.optimization_barrier(jnp.sum(qfull * kpart[:, :, None, :], axis=-1)) * inv_root
        top = jnp.maximum(lax.optimization_barrier(jnp.max(scores, axis=-1)), new_score)
        weights = jnp.exp(scores - top[..., None])
        new_weight = jnp.exp(new_score - top)
        total = lax.optimization_barrier(jnp.sum(weights, axis=-1)) + new_weight
        bweights = weights.astype(jnp.bfloat16).astype(jnp.float32)
        summed = jnp.einsum('rkgs,rskd->rkgd', bweights, values, precision=lax.Precision.HIGHEST)
        summed = summed + new_weight[..., None] * vpart[:, :, None, :]
        return (summed / total[..., None]).astype(jnp.bfloat16)
    attended = lax.map(one_batch, (group_queries, rkey, value_new, cache, lengths))
    attended = attended.reshape(MICRO_BATCHES * BATCH_ROLLOUTS, QUERY_HEADS * HEAD_SIZE)
    projected = jnp.dot(attended, w_out, preferred_element_type=jnp.float32).reshape(MICRO_BATCHES, BATCH_ROLLOUTS, MODEL_WIDTH)
    return (x_full + projected).astype(jnp.bfloat16)
```

```python
import functools

import jax
import jax.numpy as jnp
from jax import lax
from jax.experimental import pallas as pl
from jax.experimental.pallas import tpu as pltpu
from jax.sharding import PartitionSpec as P

HEAD_SIZE = 128
LANES = 128
VMEM = pl.BlockSpec(memory_space=pltpu.VMEM)
SMEM = pl.BlockSpec(memory_space=pltpu.SMEM)
ANY = pl.BlockSpec(memory_space=pl.ANY)
HBM = pl.BlockSpec(memory_space=pltpu.HBM)
F32 = jnp.float32
BF16 = jnp.bfloat16


def exchange(value, axis, size, step):
    return lax.ppermute(value, axis, [(i, i ^ step) for i in range(size)])


def in_hbm(value):
    return pltpu.with_memory_space_constraint(value, pltpu.HBM)


def params(mib):
    return pltpu.CompilerParams(vmem_limit_bytes=mib * 2**20)


def project_kernel(chunks, gx, position, tokens, gain, wq_hbm, wkv_hbm, *refs):
    outs = refs[:gx]
    wq, wkv, normed, sums, staged, sems = refs[gx:]
    depth = wq.shape[0] // chunks
    copies = []
    for c in range(chunks):
        part = (pl.ds(c * depth, depth), slice(None))
        copies.append(
            (
                pltpu.make_async_copy(wq_hbm.at[part], wq.at[part], sems.at[0, c]),
                pltpu.make_async_copy(wkv_hbm.at[part], wkv.at[part], sems.at[1, c]),
            )
        )
        for copy in copies[-1]:
            copy.start()
    batches, rows, width = tokens.shape
    total = batches * rows
    queries = wq.shape[1]
    keyvals = wkv.shape[1]
    x_full = tokens[...].astype(F32)
    squares = jnp.sum(x_full * x_full, axis=-1, keepdims=True).reshape(total, 1)
    sums[:, queries + keyvals :] = jnp.broadcast_to(squares, (total, LANES))
    scaled = (x_full * gain[...].astype(F32)).astype(BF16)
    normed[...] = scaled.reshape(total, width)
    for c in range(chunks):
        for copy in copies[c]:
            copy.wait()
        left = normed[:, c * depth : (c + 1) * depth]
        for weights, start, stop in ((wq, 0, queries), (wkv, queries, queries + keyvals)):
            part = jnp.dot(
                left, weights[c * depth : (c + 1) * depth, :], preferred_element_type=F32
            )
            if c == 0:
                sums[:, start:stop] = part
            else:
                sums[:, start:stop] += part
    here = rows // gx
    for place in range(gx):
        for m in range(batches):
            first = m * rows + place * here
            staged[place, m * here : (m + 1) * here, :] = sums[first : first + here, :]
    for k in range(gx):
        outs[k][...] = staged[position[0] ^ k]


def project(position, tokens, gain, wq, wkv, gx):
    batches, rows, width = tokens.shape
    columns = wq.shape[1] + wkv.shape[1] + LANES
    chunks = max(1, width // 256)
    return pl.pallas_call(
        functools.partial(project_kernel, chunks, gx),
        out_shape=[jax.ShapeDtypeStruct((batches * rows // gx, columns), F32)] * gx,
        in_specs=[SMEM, VMEM, VMEM, HBM, HBM],
        out_specs=[VMEM] * gx,
        scratch_shapes=[
            pltpu.VMEM(wq.shape, BF16),
            pltpu.VMEM(wkv.shape, BF16),
            pltpu.VMEM((batches * rows, width), BF16),
            pltpu.VMEM((batches * rows, columns), F32),
            pltpu.VMEM((gx, batches * rows // gx, columns), F32),
            pltpu.SemaphoreType.DMA((2, chunks)),
        ],
        compiler_params=params(24),
        name="project",
    )(position, tokens, gain, wq, wkv)


def stage_kernel(sent, cache_hbm, w_hbm, cache, weights, sems):
    del sent
    copies = [
        pltpu.make_async_copy(cache_hbm, cache, sems.at[0]),
        pltpu.make_async_copy(w_hbm.at[pl.ds(0, weights.shape[0])], weights, sems.at[1]),
    ]
    for copy in copies:
        copy.start()
    for copy in copies:
        copy.wait()


def stage(sent, cache, w_out, rows):
    return pl.pallas_call(
        stage_kernel,
        out_shape=[
            pltpu.VMEM(cache.shape, BF16),
            pltpu.VMEM((rows, w_out.shape[1]), BF16),
        ],
        in_specs=[ANY, HBM, HBM],
        out_specs=[VMEM, VMEM],
        scratch_shapes=[pltpu.SemaphoreType.DMA((2,))],
        compiler_params=params(1),
        name="stage",
    )(sent, cache, w_out)


def attend_kernel(model_width, parts, first, lengths, angles, *refs):
    received = refs[:parts]
    cache, w_hbm, out, weights_out, table, sem = refs[parts:]
    rows = cache.shape[0]
    load = pltpu.make_async_copy(
        w_hbm.at[pl.ds(first, weights_out.shape[0])], weights_out, sem
    )
    load.start()
    half = HEAD_SIZE // 2
    group = out.shape[1] // HEAD_SIZE
    queries = group * HEAD_SIZE
    sums = received[0][...]
    for k in range(1, parts):
        sums = sums + received[k][...]
    scale = lax.rsqrt(sums[:, queries + 2 * HEAD_SIZE :] / model_width + 1e-05)
    cosine = angles[0]
    sine = angles[1]

    def rotate(vectors):
        return vectors * cosine + pltpu.roll(vectors, half, 1) * sine

    def column(start):
        return sums[:, start : start + HEAD_SIZE] * scale

    for h in range(group):
        table[pl.ds(h, rows, stride=group), :] = rotate(column(h * HEAD_SIZE))
    rkey = rotate(column(queries))
    value_new = column(queries + HEAD_SIZE)
    inv_root = 1.0 / jnp.sqrt(jnp.float32(HEAD_SIZE))
    for r in range(rows):
        query = table[r * group : (r + 1) * group, :].astype(BF16)
        pairs = cache[r]
        scores = (
            lax.dot_general(query, pairs, (((1,), (1,)), ((), ())), preferred_element_type=F32)
            * inv_root
        )
        place = lax.broadcasted_iota(jnp.int32, scores.shape, 1)
        valid = jnp.logical_and(place < 2 * lengths[r], (place & 1) == 0)
        scores = jnp.where(valid, scores, -1e30)
        new_score = (
            jnp.sum(query.astype(F32) * rkey[r : r + 1, :], axis=-1, keepdims=True) * inv_root
        )
        top = jnp.maximum(jnp.max(scores, axis=-1, keepdims=True), new_score)
        weights = jnp.exp(scores - top)
        new_weight = jnp.exp(new_score - top)
        total = jnp.sum(weights, axis=-1, keepdims=True) + new_weight
        weights = pltpu.roll(weights, 1, 1).astype(BF16)
        summed = jnp.dot(weights, pairs, preferred_element_type=F32)
        summed = summed + new_weight * value_new[r : r + 1, :]
        table[r * group : (r + 1) * group, :] = summed / total
    for h in range(group):
        out[:, h * HEAD_SIZE : (h + 1) * HEAD_SIZE] = table[
            pl.ds(h, rows, stride=group), :
        ].astype(BF16)
    load.wait()


def attend(model_width, lengths, angles, received, cache, queries, w_out, first, count):
    rows = cache.shape[0]
    return pl.pallas_call(
        functools.partial(attend_kernel, model_width, len(received), first),
        out_shape=[
            jax.ShapeDtypeStruct((rows, queries), BF16),
            pltpu.VMEM((count, w_out.shape[1]), BF16),
        ],
        in_specs=[SMEM, VMEM] + [VMEM] * len(received) + [VMEM, HBM],
        out_specs=[VMEM, VMEM],
        scratch_shapes=[
            pltpu.VMEM((rows * queries // HEAD_SIZE, HEAD_SIZE), F32),
            pltpu.SemaphoreType.DMA,
        ],
        compiler_params=params(4),
        name="attend",
    )(lengths, angles, *received, cache, w_out)


def output_kernel(chunks, gx, batches, position, *refs):
    received = refs[:gx]
    begun, middle, w_hbm, out, weights, blocks, left, sems = refs[gx:]
    first = begun.shape[0] + middle.shape[0]
    depth = weights.shape[0] // chunks
    copies = []
    for c in range(chunks):
        copies.append(
            pltpu.make_async_copy(
                w_hbm.at[pl.ds(first + c * depth, depth)],
                weights.at[pl.ds(c * depth, depth)],
                sems.at[c],
            )
        )
        copies[-1].start()
    here = received[0].shape[0] // batches
    rows = here * gx
    for k in range(gx):
        blocks[position[0] ^ k] = received[k][...].astype(F32)
    for place in range(gx):
        for m in range(batches):
            start = m * rows + place * here
            left[start : start + here, :] = blocks[place, m * here : (m + 1) * here, :]

    def product(start, ref, stop):
        return jnp.dot(
            left[:, start : start + stop].astype(BF16), ref, preferred_element_type=F32
        )

    out[...] = product(0, begun[...], begun.shape[0])
    out[...] += product(begun.shape[0], middle[...], middle.shape[0])
    for c in range(chunks):
        copies[c].wait()
        out[...] += product(
            first + c * depth, weights[c * depth : (c + 1) * depth, :], depth
        )


def output(position, received, begun, middle, w_out, batches):
    gx = len(received)
    rows = received[0].shape[0] * gx
    rest = w_out.shape[0] - begun.shape[0] - middle.shape[0]
    chunks = max(1, rest // 256)
    return pl.pallas_call(
        functools.partial(output_kernel, chunks, gx, batches),
        out_shape=jax.ShapeDtypeStruct((rows, w_out.shape[1]), F32),
        in_specs=[SMEM] + [VMEM] * (gx + 2) + [HBM],
        out_specs=VMEM,
        scratch_shapes=[
            pltpu.VMEM((rest, w_out.shape[1]), BF16),
            pltpu.VMEM((gx, rows // gx, w_out.shape[0]), F32),
            pltpu.VMEM((rows, w_out.shape[0]), F32),
            pltpu.SemaphoreType.DMA((chunks,)),
        ],
        compiler_params=params(8),
        name="output",
    )(position, *received, begun, middle, w_out)


def rotation(lengths):
    half = HEAD_SIZE // 2
    freq = 500000.0 ** (-2.0 * jnp.arange(half, dtype=F32) / HEAD_SIZE)
    angle = lengths.reshape(-1, 1).astype(F32) * freq
    cosine = jnp.cos(angle)
    sine = jnp.sin(angle)
    return jnp.stack(
        [jnp.concatenate([cosine, cosine], axis=-1), jnp.concatenate([-sine, sine], axis=-1)]
    )


def add_heads(value, axis, size):
    step = 1
    while step < size:
        if step > 1:
            value = value.astype(BF16)
        other = exchange(value, axis, size, step)
        value = value.astype(F32) + other.astype(F32)
        step *= 2
    return value


def local(gx, gy, tokens, lengths, norm_gain, w_query, key_value_weight, w_out, cache):
    batches, rows, width = tokens.shape
    queries = w_query.shape[1]
    wkv = in_hbm(key_value_weight.reshape(width, -1))
    w_query = in_hbm(w_query)
    w_out = in_hbm(w_out)
    pairs = in_hbm(cache.reshape(-1, 2 * cache.shape[2], HEAD_SIZE))
    position = lax.axis_index("gx").reshape(1)
    sent = project(position, tokens, norm_gain.reshape(1, -1), w_query, wkv, gx)
    received = [sent[0]] + [exchange(sent[k], "gx", gx, k) for k in reversed(range(1, gx))]
    angles = rotation(lengths)
    depth = w_out.shape[0]
    pairs, begun = stage(sent[0], pairs, w_out, depth // 4)
    attended, middle = attend(
        width * gx, lengths.reshape(-1), angles, received, pairs, queries, w_out, depth // 4, depth // 2
    )
    gathered = {k: exchange(attended, "gx", gx, k) for k in reversed(range(1, gx))}
    gathered[0] = attended
    projected = output(
        position, [gathered[k] for k in range(gx)], begun, middle, w_out, batches
    )
    summed = add_heads(projected, "gy", gy).reshape(tokens.shape)
    return (tokens.astype(F32) + summed).astype(BF16)


def rotate(vectors, positions):
    half = vectors.shape[-1] // 2
    freq = 500000.0 ** (-2.0 * jnp.arange(half, dtype=F32) / vectors.shape[-1])
    angle = positions[..., None] * freq
    cosine = jnp.cos(angle)
    sine = jnp.sin(angle)
    first = vectors[..., :half]
    second = vectors[..., half:]
    return jnp.concatenate(
        [first * cosine - second * sine, second * cosine + first * sine], axis=-1
    )


def attend_wide(model_width, query_sum, keyval_sum, local_squares, lengths, cache):
    batches, rows_here = lengths.shape
    score_scale = lax.rsqrt(local_squares / model_width + 1e-05)
    heads_kv = keyval_sum.shape[2]
    query_group = query_sum.shape[2] // (heads_kv * HEAD_SIZE)
    query = (
        query_sum.reshape(batches, rows_here, heads_kv, query_group, HEAD_SIZE)
        * score_scale[:, :, None, None, None]
    )
    key_value = keyval_sum * score_scale[:, :, None, None]
    positions = lengths.astype(F32)
    rotated_query = rotate(query, positions[:, :, None, None]).astype(BF16)
    rkey = rotate(key_value[..., :HEAD_SIZE], positions[:, :, None])
    value_new = key_value[..., HEAD_SIZE:]
    inv_root = 1.0 / jnp.sqrt(jnp.float32(HEAD_SIZE))
    keys = cache[:, :, :, :, 0, :]
    values = cache[:, :, :, :, 1, :]
    scores = (
        jnp.einsum("mrkgd,mrskd->mrkgs", rotated_query, keys, preferred_element_type=F32)
        * inv_root
    )
    valid = jnp.arange(cache.shape[2], dtype=jnp.int32)[None, None, :] < lengths[:, :, None]
    scores = jnp.where(valid[:, :, None, None, :], scores, -1e30)
    new_score = jnp.sum(rotated_query.astype(F32) * rkey[:, :, :, None, :], axis=-1) * inv_root
    top = jnp.maximum(jnp.max(scores, axis=-1), new_score)
    weights = jnp.exp(scores - top[..., None])
    new_weight = jnp.exp(new_score - top)
    total = jnp.sum(weights, axis=-1) + new_weight
    summed = jnp.einsum(
        "mrkgs,mrskd->mrkgd", weights.astype(BF16), values, preferred_element_type=F32
    )
    summed = summed + new_weight[..., None] * value_new[:, :, :, None, :]
    return (
        (summed / total[..., None])
        .astype(BF16)
        .reshape(batches, rows_here, heads_kv * query_group * HEAD_SIZE)
    )


def local_wide(gx, tokens, lengths, norm_gain, w_query, key_value_weight, w_out, cache):
    x_full = tokens.astype(F32)
    squares = jnp.sum(x_full * x_full, axis=-1)
    normed = (x_full * norm_gain.astype(F32)).astype(BF16)
    query_part = jnp.einsum("mrd,dc->mrc", normed, w_query, preferred_element_type=F32)
    keyval_part = jnp.einsum("mrd,dkc->mrkc", normed, key_value_weight, preferred_element_type=F32)
    query_sum, keyval_sum, local_squares = (
        lax.psum_scatter(query_part, "gx", scatter_dimension=1, tiled=True),
        lax.psum_scatter(keyval_part, "gx", scatter_dimension=1, tiled=True),
        lax.psum_scatter(squares, "gx", scatter_dimension=1, tiled=True),
    )
    attended = attend_wide(
        tokens.shape[-1] * gx, query_sum, keyval_sum, local_squares, lengths, cache
    )
    projected = jnp.einsum(
        "mrc,cd->mrd",
        lax.all_gather(attended, "gx", axis=1, tiled=True),
        w_out,
        preferred_element_type=F32,
    )
    return (x_full + lax.psum(projected, "gy")).astype(BF16)


def solution(mesh):
    gx, gy = mesh.shape["gx"], mesh.shape["gy"]
    placed = (
        P(None, "groups", "gx"),
        P(None, ("groups", "gx")),
        P("gx"),
        P("gx", "gy"),
        P("gx", "gy", None),
        P("gy", "gx"),
        P(None, ("groups", "gx"), None, "gy", None, None),
    )

    def run(*args):
        kv_heads_here = args[4].shape[1]
        direct = gx <= 8 and gx & (gx - 1) == 0 and gy & (gy - 1) == 0 and kv_heads_here == 1
        if direct:
            return local(gx, gy, *args)
        return local_wide(gx, *args)

    return jax.shard_map(
        run, mesh=mesh, in_specs=placed, out_specs=P(None, "groups", "gx"), check_vma=False
    )
```

```python
import functools

import jax
import jax.numpy as jnp
from jax import lax
from jax.experimental import pallas as pl
from jax.experimental.pallas import tpu as pltpu
from jax.sharding import PartitionSpec as P

HEAD_SIZE = 128
LANES = 128
VMEM = pl.BlockSpec(memory_space=pltpu.VMEM)
SMEM = pl.BlockSpec(memory_space=pltpu.SMEM)
ANY = pl.BlockSpec(memory_space=pl.ANY)
HBM = pl.BlockSpec(memory_space=pltpu.HBM)
F32 = jnp.float32
BF16 = jnp.bfloat16


def exchange(value, axis, size, step):
    return lax.ppermute(value, axis, [(i, i ^ step) for i in range(size)])


def in_hbm(value):
    return pltpu.with_memory_space_constraint(value, pltpu.HBM)


def params(mib):
    return pltpu.CompilerParams(vmem_limit_bytes=mib * 2**20)


def project_kernel(chunks, gx, position, tokens_hbm, gain_hbm, wq_hbm, wkv_hbm, cache_hbm, *refs):
    outs = refs[:gx]
    cache, tokens, gain, wq, wkv, normed, sums, staged, small_sems, sems = refs[gx:]
    depth = wq.shape[0] // chunks
    small = [
        pltpu.make_async_copy(tokens_hbm, tokens, small_sems.at[0]),
        pltpu.make_async_copy(gain_hbm, gain, small_sems.at[1]),
        pltpu.make_async_copy(cache_hbm, cache, small_sems.at[2]),
    ]
    small[0].start()
    small[1].start()

    def chunk(c):
        part = (pl.ds(c * depth, depth), slice(None))
        return (
            pltpu.make_async_copy(wq_hbm.at[part], wq.at[part], sems.at[0, c]),
            pltpu.make_async_copy(wkv_hbm.at[part], wkv.at[part], sems.at[1, c]),
        )

    @pl.loop(0, chunks)
    def _(c):
        for copy in chunk(c):
            copy.start()

    small[0].wait()
    small[1].wait()
    batches, rows, width = tokens.shape
    total = batches * rows
    queries = wq.shape[1]
    keyvals = wkv.shape[1]
    x_full = tokens[...].astype(F32)
    squares = jnp.sum(x_full * x_full, axis=-1, keepdims=True).reshape(total, 1)
    sums[:, queries + keyvals :] = jnp.broadcast_to(squares, (total, LANES))
    scaled = (x_full * gain[...].astype(F32)).astype(BF16)
    normed[...] = scaled.reshape(total, width)
    for c in range(chunks):
        if c == max(0, chunks - 3):
            small[2].start()
        for copy in chunk(c):
            copy.wait()
        left = normed[:, c * depth : (c + 1) * depth]
        for weights, start, stop in ((wq, 0, queries), (wkv, queries, queries + keyvals)):
            part = jnp.dot(
                left, weights[c * depth : (c + 1) * depth, :], preferred_element_type=F32
            )
            if c == 0:
                sums[:, start:stop] = part
            else:
                sums[:, start:stop] += part
    here = rows // gx
    for place in range(gx):
        for m in range(batches):
            first = m * rows + place * here
            staged[place, m * here : (m + 1) * here, :] = sums[first : first + here, :]
    for k in range(gx):
        outs[k][...] = staged[position[0] ^ k]
    small[2].wait()


def project(position, tokens, gain, wq, wkv, cache, gx):
    batches, rows, width = tokens.shape
    columns = wq.shape[1] + wkv.shape[1] + LANES
    chunks = max(1, width // 256)
    return pl.pallas_call(
        functools.partial(project_kernel, chunks, gx),
        out_shape=[jax.ShapeDtypeStruct((batches * rows // gx, columns), F32)] * gx
        + [pltpu.VMEM(cache.shape, BF16)],
        in_specs=[SMEM] + [HBM] * 5,
        out_specs=[VMEM] * (gx + 1),
        scratch_shapes=[
            pltpu.VMEM(tokens.shape, BF16),
            pltpu.VMEM(gain.shape, BF16),
            pltpu.VMEM(wq.shape, BF16),
            pltpu.VMEM(wkv.shape, BF16),
            pltpu.VMEM((batches * rows, width), BF16),
            pltpu.VMEM((batches * rows, columns), F32),
            pltpu.VMEM((gx, batches * rows // gx, columns), F32),
            pltpu.SemaphoreType.DMA((3,)),
            pltpu.SemaphoreType.DMA((2, chunks)),
        ],
        compiler_params=params(32),
        name="project",
    )(position, tokens, gain, wq, wkv, cache)


def stage_kernel(first, after, w_hbm, weights, sems):
    del after
    pieces = sems.shape[0]
    depth = weights.shape[0] // pieces

    def piece(c):
        return pltpu.make_async_copy(
            w_hbm.at[pl.ds(first + c * depth, depth)],
            weights.at[pl.ds(c * depth, depth)],
            sems.at[c],
        )

    for c in range(pieces):
        piece(c).start()
    for c in range(pieces):
        piece(c).wait()


def stage(after, w_out, first, rows):
    return pl.pallas_call(
        functools.partial(stage_kernel, first),
        out_shape=pltpu.VMEM((rows, w_out.shape[1]), BF16),
        in_specs=[ANY, HBM],
        out_specs=VMEM,
        scratch_shapes=[pltpu.SemaphoreType.DMA((2,))],
        compiler_params=params(1),
        name="stage",
    )(after, w_out)


def attend_kernel(model_width, parts, first, lengths, angles, *refs):
    received = refs[:parts]
    cache, staged, w_hbm, out, weights_out, table, sem = refs[parts:]
    del staged
    rows = cache.shape[0]
    pieces = sem.shape[0]
    depth = weights_out.shape[0] // pieces

    def load(c):
        return pltpu.make_async_copy(
            w_hbm.at[pl.ds(first + c * depth, depth)],
            weights_out.at[pl.ds(c * depth, depth)],
            sem.at[c],
        )

    @pl.loop(0, pieces)
    def _(c):
        load(c).start()

    half = HEAD_SIZE // 2
    group = out.shape[1] // HEAD_SIZE
    queries = group * HEAD_SIZE
    sums = received[0][...]
    for k in range(1, parts):
        sums = sums + received[k][...]
    scale = lax.rsqrt(sums[:, queries + 2 * HEAD_SIZE :] / model_width + 1e-05)
    cosine = angles[0]
    sine = angles[1]

    def rotate(vectors):
        return vectors * cosine + pltpu.roll(vectors, half, 1) * sine

    def column(start):
        return sums[:, start : start + HEAD_SIZE] * scale

    for h in range(group):
        table[pl.ds(h, rows, stride=group), :] = rotate(column(h * HEAD_SIZE))
    rkey = rotate(column(queries))
    value_new = column(queries + HEAD_SIZE)
    inv_root = 1.0 / jnp.sqrt(jnp.float32(HEAD_SIZE))
    pair = 2 if rows % 2 == 0 else 1
    for r in range(0, rows, pair):
        members = range(r, r + pair)
        query = table[r * group : (r + pair) * group, :]
        block = lax.broadcasted_iota(jnp.int32, (pair * group, 1), 0) // group
        left = jnp.concatenate([jnp.where(block == j, query, 0.0) for j in range(pair)], axis=1)
        right = jnp.concatenate([cache[n] for n in members], axis=1)
        scores = (
            lax.dot_general(
                left.astype(BF16), right, (((1,), (1,)), ((), ())), preferred_element_type=F32
            )
            * inv_root
        )
        limit = jnp.where(block == 0, lengths[r], lengths[r + pair - 1])
        place = lax.broadcasted_iota(jnp.int32, scores.shape, 1)
        valid = jnp.logical_and(place < 2 * limit, (place & 1) == 0)
        scores = jnp.where(valid, scores, -1e30)

        def spread(vectors):
            return jnp.where(
                block == 0, vectors[r : r + 1, :], vectors[r + pair - 1 : r + pair, :]
            )

        new_score = (
            jnp.sum(query.astype(BF16).astype(F32) * spread(rkey), axis=-1, keepdims=True)
            * inv_root
        )
        top = jnp.maximum(jnp.max(scores, axis=-1, keepdims=True), new_score)
        weights = jnp.exp(scores - top)
        new_weight = jnp.exp(new_score - top)
        total = jnp.sum(weights, axis=-1, keepdims=True) + new_weight
        weights = pltpu.roll(weights, 1, 1).astype(BF16)
        both = jnp.dot(weights, right, preferred_element_type=F32)
        summed = both[:, :HEAD_SIZE]
        for j in range(1, pair):
            summed = jnp.where(block == j, both[:, j * HEAD_SIZE : (j + 1) * HEAD_SIZE], summed)
        summed = summed + new_weight * spread(value_new)
        table[r * group : (r + pair) * group, :] = summed / total
    for h in range(group):
        out[:, h * HEAD_SIZE : (h + 1) * HEAD_SIZE] = table[
            pl.ds(h, rows, stride=group), :
        ].astype(BF16)
    for c in range(pieces):
        load(c).wait()


def attend(model_width, lengths, angles, received, cache, queries, staged, w_out, count):
    first = staged.shape[0]
    rows = cache.shape[0]
    return pl.pallas_call(
        functools.partial(attend_kernel, model_width, len(received), first),
        out_shape=[
            jax.ShapeDtypeStruct((rows, queries), BF16),
            pltpu.VMEM((count, w_out.shape[1]), BF16),
        ],
        in_specs=[SMEM, VMEM] + [VMEM] * len(received) + [VMEM, ANY, HBM],
        out_specs=[VMEM, VMEM],
        scratch_shapes=[
            pltpu.VMEM((rows * queries // HEAD_SIZE, HEAD_SIZE), F32),
            pltpu.SemaphoreType.DMA((4,)),
        ],
        compiler_params=params(4),
        name="attend",
    )(lengths, angles, *received, cache, staged, w_out)


def output_kernel(chunks, gx, batches, position, *refs):
    received = refs[:gx]
    staged = refs[gx:-6]
    w_hbm, out, weights, blocks, left, sems = refs[-6:]
    first = sum(ref.shape[0] for ref in staged)
    depth = weights.shape[0] // chunks

    def load(c):
        return pltpu.make_async_copy(
            w_hbm.at[pl.ds(first + c * depth, depth)],
            weights.at[pl.ds(c * depth, depth)],
            sems.at[c],
        )

    @pl.loop(0, chunks)
    def _(c):
        load(c).start()

    here = received[0].shape[0] // batches
    rows = here * gx
    for k in range(gx):
        blocks[position[0] ^ k] = received[k][...].astype(F32)
    for place in range(gx):
        for m in range(batches):
            start = m * rows + place * here
            left[start : start + here, :] = blocks[place, m * here : (m + 1) * here, :]

    def product(start, ref, stop):
        return jnp.dot(
            left[:, start : start + stop].astype(BF16), ref, preferred_element_type=F32
        )

    start = 0
    for ref in staged:
        part = product(start, ref[...], ref.shape[0])
        if start == 0:
            out[...] = part
        else:
            out[...] += part
        start += ref.shape[0]
    for c in range(chunks):
        load(c).wait()
        out[...] += product(
            first + c * depth, weights[c * depth : (c + 1) * depth, :], depth
        )


def output(position, received, staged, w_out, batches):
    gx = len(received)
    rows = received[0].shape[0] * gx
    rest = w_out.shape[0] - sum(ref.shape[0] for ref in staged)
    chunks = max(1, rest // 256)
    return pl.pallas_call(
        functools.partial(output_kernel, chunks, gx, batches),
        out_shape=jax.ShapeDtypeStruct((rows, w_out.shape[1]), F32),
        in_specs=[SMEM] + [VMEM] * (gx + len(staged)) + [HBM],
        out_specs=VMEM,
        scratch_shapes=[
            pltpu.VMEM((rest, w_out.shape[1]), BF16),
            pltpu.VMEM((gx, rows // gx, w_out.shape[0]), F32),
            pltpu.VMEM((rows, w_out.shape[0]), F32),
            pltpu.SemaphoreType.DMA((chunks,)),
        ],
        compiler_params=params(24),
        name="output",
    )(position, *received, *staged, w_out)


def rotation(lengths):
    half = HEAD_SIZE // 2
    freq = 500000.0 ** (-2.0 * jnp.arange(half, dtype=F32) / HEAD_SIZE)
    angle = lengths.reshape(-1, 1).astype(F32) * freq
    cosine = jnp.cos(angle)
    sine = jnp.sin(angle)
    return jnp.stack(
        [jnp.concatenate([cosine, cosine], axis=-1), jnp.concatenate([-sine, sine], axis=-1)]
    )


def add_heads(value, axis, size):
    step = 1
    while step < size:
        if step > 1:
            value = value.astype(BF16)
        other = exchange(value, axis, size, step)
        value = value.astype(F32) + other.astype(F32)
        step *= 2
    return value


def local(gx, gy, tokens, lengths, norm_gain, w_query, key_value_weight, w_out, cache):
    batches, rows, width = tokens.shape
    queries = w_query.shape[1]
    wkv = in_hbm(key_value_weight.reshape(width, -1))
    w_query = in_hbm(w_query)
    w_out = in_hbm(w_out)
    pairs = in_hbm(cache.reshape(-1, 2 * cache.shape[2], HEAD_SIZE))
    position = lax.axis_index("gx").reshape(1)
    *sent, pairs = project(position, in_hbm(tokens), in_hbm(norm_gain), w_query, wkv, pairs, gx)
    received = [sent[0]] + [exchange(sent[k], "gx", gx, k) for k in reversed(range(1, gx))]
    angles = rotation(lengths)
    depth = w_out.shape[0] // 16
    begun = stage(sent[0], w_out, 0, 4 * depth)
    attended, middle = attend(
        width * gx, lengths.reshape(-1), angles, received, pairs, queries, begun, w_out, 4 * depth
    )
    last = stage(attended, w_out, 8 * depth, 6 * depth)
    gathered = {k: exchange(attended, "gx", gx, k) for k in reversed(range(1, gx))}
    gathered[0] = attended
    projected = output(
        position, [gathered[k] for k in range(gx)], [begun, middle, last], w_out, batches
    )
    summed = add_heads(projected, "gy", gy).reshape(tokens.shape)
    return (tokens.astype(F32) + summed).astype(BF16)


def rotate(vectors, positions):
    half = vectors.shape[-1] // 2
    freq = 500000.0 ** (-2.0 * jnp.arange(half, dtype=F32) / vectors.shape[-1])
    angle = positions[..., None] * freq
    cosine = jnp.cos(angle)
    sine = jnp.sin(angle)
    first = vectors[..., :half]
    second = vectors[..., half:]
    return jnp.concatenate(
        [first * cosine - second * sine, second * cosine + first * sine], axis=-1
    )


def attend_wide(model_width, query_sum, keyval_sum, local_squares, lengths, cache):
    batches, rows_here = lengths.shape
    score_scale = lax.rsqrt(local_squares / model_width + 1e-05)
    heads_kv = keyval_sum.shape[2]
    query_group = query_sum.shape[2] // (heads_kv * HEAD_SIZE)
    query = (
        query_sum.reshape(batches, rows_here, heads_kv, query_group, HEAD_SIZE)
        * score_scale[:, :, None, None, None]
    )
    key_value = keyval_sum * score_scale[:, :, None, None]
    positions = lengths.astype(F32)
    rotated_query = rotate(query, positions[:, :, None, None]).astype(BF16)
    rkey = rotate(key_value[..., :HEAD_SIZE], positions[:, :, None])
    value_new = key_value[..., HEAD_SIZE:]
    inv_root = 1.0 / jnp.sqrt(jnp.float32(HEAD_SIZE))
    keys = cache[:, :, :, :, 0, :]
    values = cache[:, :, :, :, 1, :]
    scores = (
        jnp.einsum("mrkgd,mrskd->mrkgs", rotated_query, keys, preferred_element_type=F32)
        * inv_root
    )
    valid = jnp.arange(cache.shape[2], dtype=jnp.int32)[None, None, :] < lengths[:, :, None]
    scores = jnp.where(valid[:, :, None, None, :], scores, -1e30)
    new_score = jnp.sum(rotated_query.astype(F32) * rkey[:, :, :, None, :], axis=-1) * inv_root
    top = jnp.maximum(jnp.max(scores, axis=-1), new_score)
    weights = jnp.exp(scores - top[..., None])
    new_weight = jnp.exp(new_score - top)
    total = jnp.sum(weights, axis=-1) + new_weight
    summed = jnp.einsum(
        "mrkgs,mrskd->mrkgd", weights.astype(BF16), values, preferred_element_type=F32
    )
    summed = summed + new_weight[..., None] * value_new[:, :, :, None, :]
    return (
        (summed / total[..., None])
        .astype(BF16)
        .reshape(batches, rows_here, heads_kv * query_group * HEAD_SIZE)
    )


def local_wide(gx, tokens, lengths, norm_gain, w_query, key_value_weight, w_out, cache):
    x_full = tokens.astype(F32)
    squares = jnp.sum(x_full * x_full, axis=-1)
    normed = (x_full * norm_gain.astype(F32)).astype(BF16)
    query_part = jnp.einsum("mrd,dc->mrc", normed, w_query, preferred_element_type=F32)
    keyval_part = jnp.einsum("mrd,dkc->mrkc", normed, key_value_weight, preferred_element_type=F32)
    query_sum, keyval_sum, local_squares = (
        lax.psum_scatter(query_part, "gx", scatter_dimension=1, tiled=True),
        lax.psum_scatter(keyval_part, "gx", scatter_dimension=1, tiled=True),
        lax.psum_scatter(squares, "gx", scatter_dimension=1, tiled=True),
    )
    attended = attend_wide(
        tokens.shape[-1] * gx, query_sum, keyval_sum, local_squares, lengths, cache
    )
    projected = jnp.einsum(
        "mrc,cd->mrd",
        lax.all_gather(attended, "gx", axis=1, tiled=True),
        w_out,
        preferred_element_type=F32,
    )
    return (x_full + lax.psum(projected, "gy")).astype(BF16)


def solution(mesh):
    gx, gy = mesh.shape["gx"], mesh.shape["gy"]
    placed = (
        P(None, "groups", "gx"),
        P(None, ("groups", "gx")),
        P("gx"),
        P("gx", "gy"),
        P("gx", "gy", None),
        P("gy", "gx"),
        P(None, ("groups", "gx"), None, "gy", None, None),
    )

    def run(*args):
        kv_heads_here = args[4].shape[1]
        direct = gx <= 8 and gx & (gx - 1) == 0 and gy & (gy - 1) == 0 and kv_heads_here == 1
        if direct:
            return local(gx, gy, *args)
        return local_wide(gx, *args)

    return jax.shard_map(
        run, mesh=mesh, in_specs=placed, out_specs=P(None, "groups", "gx"), check_vma=False
    )
```

```python
import functools

import jax
import jax.numpy as jnp
from jax import lax
from jax.experimental import pallas as pl
from jax.experimental.pallas import tpu as pltpu
from jax.sharding import PartitionSpec as P

HEAD_SIZE = 128
LANES = 128
VMEM = pl.BlockSpec(memory_space=pltpu.VMEM)
SMEM = pl.BlockSpec(memory_space=pltpu.SMEM)
ANY = pl.BlockSpec(memory_space=pl.ANY)
HBM = pl.BlockSpec(memory_space=pltpu.HBM)
F32 = jnp.float32
BF16 = jnp.bfloat16


def exchange(value, axis, size, step):
    return lax.ppermute(value, axis, [(i, i ^ step) for i in range(size)])


def in_hbm(value):
    return pltpu.with_memory_space_constraint(value, pltpu.HBM)


def params(mib):
    return pltpu.CompilerParams(vmem_limit_bytes=mib * 2**20)


def project_kernel(chunks, gx, position, tokens_hbm, gain_hbm, wq_hbm, wkv_hbm, *refs):
    outs = refs[:gx]
    tokens, gain, wq, wkv, normed, sums, staged, small_sems, sems = refs[gx:]
    depth = wq.shape[0] // chunks
    small = [
        pltpu.make_async_copy(tokens_hbm, tokens, small_sems.at[0]),
        pltpu.make_async_copy(gain_hbm, gain, small_sems.at[1]),
    ]
    small[0].start()
    small[1].start()

    def chunk(c):
        part = (pl.ds(c * depth, depth), slice(None))
        return (
            pltpu.make_async_copy(wq_hbm.at[part], wq.at[part], sems.at[0, c]),
            pltpu.make_async_copy(wkv_hbm.at[part], wkv.at[part], sems.at[1, c]),
        )

    @pl.loop(0, chunks)
    def _(c):
        for copy in chunk(c):
            copy.start()

    small[0].wait()
    small[1].wait()
    batches, rows, width = tokens.shape
    total = batches * rows
    queries = wq.shape[1]
    keyvals = wkv.shape[1]
    x_full = tokens[...].astype(F32)
    squares = jnp.sum(x_full * x_full, axis=-1, keepdims=True).reshape(total, 1)
    sums[:, queries + keyvals :] = jnp.broadcast_to(squares, (total, LANES))
    scaled = (x_full * gain[...].astype(F32)).astype(BF16)
    normed[...] = scaled.reshape(total, width)
    for c in range(chunks):
        for copy in chunk(c):
            copy.wait()
        left = normed[:, c * depth : (c + 1) * depth]
        for weights, start, stop in ((wq, 0, queries), (wkv, queries, queries + keyvals)):
            part = jnp.dot(
                left, weights[c * depth : (c + 1) * depth, :], preferred_element_type=F32
            )
            if c == 0:
                sums[:, start:stop] = part
            else:
                sums[:, start:stop] += part
    here = rows // gx
    for place in range(gx):
        for m in range(batches):
            first = m * rows + place * here
            staged[place, m * here : (m + 1) * here, :] = sums[first : first + here, :]
    for k in range(gx):
        outs[k][...] = staged[position[0] ^ k]


def project(position, tokens, gain, wq, wkv, gx):
    batches, rows, width = tokens.shape
    columns = wq.shape[1] + wkv.shape[1] + LANES
    chunks = max(1, width // 256)
    return pl.pallas_call(
        functools.partial(project_kernel, chunks, gx),
        out_shape=[jax.ShapeDtypeStruct((batches * rows // gx, columns), F32)] * gx,
        in_specs=[SMEM] + [HBM] * 4,
        out_specs=[VMEM] * gx,
        scratch_shapes=[
            pltpu.VMEM(tokens.shape, BF16),
            pltpu.VMEM(gain.shape, BF16),
            pltpu.VMEM(wq.shape, BF16),
            pltpu.VMEM(wkv.shape, BF16),
            pltpu.VMEM((batches * rows, width), BF16),
            pltpu.VMEM((batches * rows, columns), F32),
            pltpu.VMEM((gx, batches * rows // gx, columns), F32),
            pltpu.SemaphoreType.DMA((2,)),
            pltpu.SemaphoreType.DMA((2, chunks)),
        ],
        compiler_params=params(32),
        name="project",
    )(position, tokens, gain, wq, wkv)


def stage_kernel(after, cache_hbm, cache, sems):
    del after
    rows = cache.shape[0]
    for r in range(rows):
        pltpu.make_async_copy(cache_hbm.at[r], cache.at[r], sems.at[r]).start()
    for r in range(rows):
        pltpu.make_async_copy(cache_hbm.at[r], cache.at[r], sems.at[r]).wait()


def stage(after, cache):
    return pl.pallas_call(
        stage_kernel,
        out_shape=pltpu.VMEM(cache.shape, BF16),
        in_specs=[ANY, HBM],
        out_specs=VMEM,
        scratch_shapes=[pltpu.SemaphoreType.DMA((cache.shape[0],))],
        compiler_params=params(1),
        name="stage",
    )(after, cache)


def attend_kernel(model_width, parts, lengths, angles, *refs):
    received = refs[:parts]
    cache, out, table = refs[parts:]
    rows = cache.shape[0]
    half = HEAD_SIZE // 2
    group = out.shape[1] // HEAD_SIZE
    queries = group * HEAD_SIZE
    sums = received[0][...]
    for k in range(1, parts):
        sums = sums + received[k][...]
    scale = lax.rsqrt(sums[:, queries + 2 * HEAD_SIZE :] / model_width + 1e-05)
    cosine = angles[0]
    sine = angles[1]

    def rotate(vectors):
        return vectors * cosine + pltpu.roll(vectors, half, 1) * sine

    def column(start):
        return sums[:, start : start + HEAD_SIZE] * scale

    for h in range(group):
        table[pl.ds(h, rows, stride=group), :] = rotate(column(h * HEAD_SIZE))
    rkey = rotate(column(queries))
    value_new = column(queries + HEAD_SIZE)
    inv_root = 1.0 / jnp.sqrt(jnp.float32(HEAD_SIZE))
    pair = 2 if rows % 2 == 0 else 1
    for r in range(0, rows, pair):
        members = range(r, r + pair)
        query = table[r * group : (r + pair) * group, :]
        block = lax.broadcasted_iota(jnp.int32, (pair * group, 1), 0) // group
        left = jnp.concatenate([jnp.where(block == j, query, 0.0) for j in range(pair)], axis=1)
        right = jnp.concatenate([cache[n] for n in members], axis=1)
        scores = (
            lax.dot_general(
                left.astype(BF16), right, (((1,), (1,)), ((), ())), preferred_element_type=F32
            )
            * inv_root
        )
        limit = jnp.where(block == 0, lengths[r], lengths[r + pair - 1])
        place = lax.broadcasted_iota(jnp.int32, scores.shape, 1)
        valid = jnp.logical_and(place < 2 * limit, (place & 1) == 0)
        scores = jnp.where(valid, scores, -1e30)

        def spread(vectors):
            return jnp.where(
                block == 0, vectors[r : r + 1, :], vectors[r + pair - 1 : r + pair, :]
            )

        new_score = (
            jnp.sum(query.astype(BF16).astype(F32) * spread(rkey), axis=-1, keepdims=True)
            * inv_root
        )
        top = jnp.maximum(jnp.max(scores, axis=-1, keepdims=True), new_score)
        weights = jnp.exp(scores - top)
        new_weight = jnp.exp(new_score - top)
        total = jnp.sum(weights, axis=-1, keepdims=True) + new_weight
        weights = pltpu.roll(weights, 1, 1).astype(BF16)
        both = jnp.dot(weights, right, preferred_element_type=F32)
        summed = both[:, :HEAD_SIZE]
        for j in range(1, pair):
            summed = jnp.where(block == j, both[:, j * HEAD_SIZE : (j + 1) * HEAD_SIZE], summed)
        summed = summed + new_weight * spread(value_new)
        table[r * group : (r + pair) * group, :] = summed / total
    for h in range(group):
        out[:, h * HEAD_SIZE : (h + 1) * HEAD_SIZE] = table[
            pl.ds(h, rows, stride=group), :
        ].astype(BF16)


def attend(model_width, lengths, angles, received, cache, queries):
    rows = cache.shape[0]
    return pl.pallas_call(
        functools.partial(attend_kernel, model_width, len(received)),
        out_shape=jax.ShapeDtypeStruct((rows, queries), BF16),
        in_specs=[SMEM, VMEM] + [VMEM] * len(received) + [VMEM],
        out_specs=VMEM,
        scratch_shapes=[
            pltpu.VMEM((rows * queries // HEAD_SIZE, HEAD_SIZE), F32),
        ],
        compiler_params=params(4),
        cost_estimate=pl.CostEstimate(flops=10000000000, bytes_accessed=0, transcendentals=0),
        name="attend",
    )(lengths, angles, *received, cache)


def output_kernel(gx, batches, position, *refs):
    received = refs[:gx]
    weights, out, blocks, left = refs[gx:]
    here = received[0].shape[0] // batches
    rows = here * gx
    for k in range(gx):
        blocks[position[0] ^ k] = received[k][...].astype(F32)
    for place in range(gx):
        for m in range(batches):
            start = m * rows + place * here
            left[start : start + here, :] = blocks[place, m * here : (m + 1) * here, :]
    out[...] = jnp.dot(left[...].astype(BF16), weights[...], preferred_element_type=F32)


def output(position, received, w_out, batches):
    gx = len(received)
    rows = received[0].shape[0] * gx
    return pl.pallas_call(
        functools.partial(output_kernel, gx, batches),
        out_shape=jax.ShapeDtypeStruct((rows, w_out.shape[1]), F32),
        in_specs=[SMEM] + [VMEM] * (gx + 1),
        out_specs=VMEM,
        scratch_shapes=[
            pltpu.VMEM((gx, rows // gx, w_out.shape[0]), F32),
            pltpu.VMEM((rows, w_out.shape[0]), F32),
        ],
        compiler_params=params(4),
        name="output",
    )(position, *received, w_out)


def rotation(lengths):
    half = HEAD_SIZE // 2
    freq = 500000.0 ** (-2.0 * jnp.arange(half, dtype=F32) / HEAD_SIZE)
    angle = lengths.reshape(-1, 1).astype(F32) * freq
    cosine = jnp.cos(angle)
    sine = jnp.sin(angle)
    return jnp.stack(
        [jnp.concatenate([cosine, cosine], axis=-1), jnp.concatenate([-sine, sine], axis=-1)]
    )


def add_heads(value, axis, size):
    step = 1
    while step < size:
        if step > 1:
            value = value.astype(BF16)
        other = exchange(value, axis, size, step)
        value = value.astype(F32) + other.astype(F32)
        step *= 2
    return value


def local(gx, gy, tokens, lengths, norm_gain, w_query, key_value_weight, w_out, cache):
    batches, rows, width = tokens.shape
    queries = w_query.shape[1]
    wkv = in_hbm(key_value_weight.reshape(width, -1))
    w_query = in_hbm(w_query)
    pairs = in_hbm(cache.reshape(-1, 2 * cache.shape[2], HEAD_SIZE))
    position = lax.axis_index("gx").reshape(1)
    sent = project(position, in_hbm(tokens), in_hbm(norm_gain), w_query, wkv, gx)
    pairs = stage(sent[0], pairs)
    received = [sent[0]] + [exchange(sent[k], "gx", gx, k) for k in reversed(range(1, gx))]
    angles = rotation(lengths)
    attended = attend(
        width * gx, lengths.reshape(-1), angles, received, pairs, queries
    )
    gathered = {k: exchange(attended, "gx", gx, k) for k in reversed(range(1, gx))}
    gathered[0] = attended
    projected = output(position, [gathered[k] for k in range(gx)], w_out, batches)
    summed = add_heads(projected, "gy", gy).reshape(tokens.shape)
    return (tokens.astype(F32) + summed).astype(BF16)


def rotate(vectors, positions):
    half = vectors.shape[-1] // 2
    freq = 500000.0 ** (-2.0 * jnp.arange(half, dtype=F32) / vectors.shape[-1])
    angle = positions[..., None] * freq
    cosine = jnp.cos(angle)
    sine = jnp.sin(angle)
    first = vectors[..., :half]
    second = vectors[..., half:]
    return jnp.concatenate(
        [first * cosine - second * sine, second * cosine + first * sine], axis=-1
    )


def attend_wide(model_width, query_sum, keyval_sum, local_squares, lengths, cache):
    batches, rows_here = lengths.shape
    score_scale = lax.rsqrt(local_squares / model_width + 1e-05)
    heads_kv = keyval_sum.shape[2]
    query_group = query_sum.shape[2] // (heads_kv * HEAD_SIZE)
    query = (
        query_sum.reshape(batches, rows_here, heads_kv, query_group, HEAD_SIZE)
        * score_scale[:, :, None, None, None]
    )
    key_value = keyval_sum * score_scale[:, :, None, None]
    positions = lengths.astype(F32)
    rotated_query = rotate(query, positions[:, :, None, None]).astype(BF16)
    rkey = rotate(key_value[..., :HEAD_SIZE], positions[:, :, None])
    value_new = key_value[..., HEAD_SIZE:]
    inv_root = 1.0 / jnp.sqrt(jnp.float32(HEAD_SIZE))
    keys = cache[:, :, :, :, 0, :]
    values = cache[:, :, :, :, 1, :]
    scores = (
        jnp.einsum("mrkgd,mrskd->mrkgs", rotated_query, keys, preferred_element_type=F32)
        * inv_root
    )
    valid = jnp.arange(cache.shape[2], dtype=jnp.int32)[None, None, :] < lengths[:, :, None]
    scores = jnp.where(valid[:, :, None, None, :], scores, -1e30)
    new_score = jnp.sum(rotated_query.astype(F32) * rkey[:, :, :, None, :], axis=-1) * inv_root
    top = jnp.maximum(jnp.max(scores, axis=-1), new_score)
    weights = jnp.exp(scores - top[..., None])
    new_weight = jnp.exp(new_score - top)
    total = jnp.sum(weights, axis=-1) + new_weight
    summed = jnp.einsum(
        "mrkgs,mrskd->mrkgd", weights.astype(BF16), values, preferred_element_type=F32
    )
    summed = summed + new_weight[..., None] * value_new[:, :, :, None, :]
    return (
        (summed / total[..., None])
        .astype(BF16)
        .reshape(batches, rows_here, heads_kv * query_group * HEAD_SIZE)
    )


def local_wide(gx, tokens, lengths, norm_gain, w_query, key_value_weight, w_out, cache):
    x_full = tokens.astype(F32)
    squares = jnp.sum(x_full * x_full, axis=-1)
    normed = (x_full * norm_gain.astype(F32)).astype(BF16)
    query_part = jnp.einsum("mrd,dc->mrc", normed, w_query, preferred_element_type=F32)
    keyval_part = jnp.einsum("mrd,dkc->mrkc", normed, key_value_weight, preferred_element_type=F32)
    query_sum, keyval_sum, local_squares = (
        lax.psum_scatter(query_part, "gx", scatter_dimension=1, tiled=True),
        lax.psum_scatter(keyval_part, "gx", scatter_dimension=1, tiled=True),
        lax.psum_scatter(squares, "gx", scatter_dimension=1, tiled=True),
    )
    attended = attend_wide(
        tokens.shape[-1] * gx, query_sum, keyval_sum, local_squares, lengths, cache
    )
    projected = jnp.einsum(
        "mrc,cd->mrd",
        lax.all_gather(attended, "gx", axis=1, tiled=True),
        w_out,
        preferred_element_type=F32,
    )
    return (x_full + lax.psum(projected, "gy")).astype(BF16)


def solution(mesh):
    gx, gy = mesh.shape["gx"], mesh.shape["gy"]
    placed = (
        P(None, "groups", "gx"),
        P(None, ("groups", "gx")),
        P("gx"),
        P("gx", "gy"),
        P("gx", "gy", None),
        P("gy", "gx"),
        P(None, ("groups", "gx"), None, "gy", None, None),
    )

    def run(*args):
        kv_heads_here = args[4].shape[1]
        direct = gx <= 8 and gx & (gx - 1) == 0 and gy & (gy - 1) == 0 and kv_heads_here == 1
        if direct:
            return local(gx, gy, *args)
        return local_wide(gx, *args)

    return jax.shard_map(
        run, mesh=mesh, in_specs=placed, out_specs=P(None, "groups", "gx"), check_vma=False
    )
```

```python
import functools

import jax
import jax.numpy as jnp
from jax import lax
from jax.experimental import pallas as pl
from jax.experimental.pallas import tpu as pltpu
from jax.sharding import PartitionSpec as P

HEAD_SIZE = 128
LANES = 128
VMEM = pl.BlockSpec(memory_space=pltpu.VMEM)
ANY = pl.BlockSpec(memory_space=pl.ANY)
HBM = pl.BlockSpec(memory_space=pltpu.HBM)
F32 = jnp.float32
BF16 = jnp.bfloat16


def exchange(value, axis, size, step):
    return lax.ppermute(value, axis, [(i, i ^ step) for i in range(size)])


def in_hbm(value):
    return pltpu.with_memory_space_constraint(value, pltpu.HBM)


def params(mib):
    return pltpu.CompilerParams(vmem_limit_bytes=mib * 2**20)


def project_kernel(chunks, gx, tokens_hbm, gain_hbm, wq_hbm, wkv_hbm, *refs):
    outs = refs[:gx]
    tokens, gain, wq, wkv, normed, sums, staged, small_sems, sems = refs[gx:]
    depth = wq.shape[0] // chunks
    small = [
        pltpu.make_async_copy(tokens_hbm, tokens, small_sems.at[0]),
        pltpu.make_async_copy(gain_hbm, gain, small_sems.at[1]),
    ]
    small[0].start()
    small[1].start()

    def chunk(c):
        part = (pl.ds(c * depth, depth), slice(None))
        return (
            pltpu.make_async_copy(wq_hbm.at[part], wq.at[part], sems.at[0, c]),
            pltpu.make_async_copy(wkv_hbm.at[part], wkv.at[part], sems.at[1, c]),
        )

    @pl.loop(0, chunks)
    def _(c):
        for copy in chunk(c):
            copy.start()

    small[0].wait()
    small[1].wait()
    batches, rows, width = tokens.shape
    total = batches * rows
    queries = wq.shape[1]
    keyvals = wkv.shape[1]
    x_full = tokens[...].astype(F32)
    squares = jnp.sum(x_full * x_full, axis=-1, keepdims=True).reshape(total, 1)
    sums[:, queries + keyvals :] = jnp.broadcast_to(squares, (total, LANES))
    scaled = (x_full * gain[...].astype(F32)).astype(BF16)
    normed[...] = scaled.reshape(total, width)
    for c in range(chunks):
        for copy in chunk(c):
            copy.wait()
        left = normed[:, c * depth : (c + 1) * depth]
        for weights, start, stop in ((wq, 0, queries), (wkv, queries, queries + keyvals)):
            part = jnp.dot(
                left, weights[c * depth : (c + 1) * depth, :], preferred_element_type=F32
            )
            if c == 0:
                sums[:, start:stop] = part
            else:
                sums[:, start:stop] += part
    here = rows // gx
    for place in range(gx):
        for m in range(batches):
            first = m * rows + place * here
            staged[place, m * here : (m + 1) * here, :] = sums[first : first + here, :]
    for k in range(gx):
        outs[k][...] = staged[lax.axis_index("gx") ^ k]


def project(tokens, gain, wq, wkv, gx):
    batches, rows, width = tokens.shape
    columns = wq.shape[1] + wkv.shape[1] + LANES
    chunks = max(1, width // 256)
    return pl.pallas_call(
        functools.partial(project_kernel, chunks, gx),
        out_shape=[jax.ShapeDtypeStruct((batches * rows // gx, columns), F32)] * gx,
        in_specs=[HBM] * 4,
        out_specs=[VMEM] * gx,
        scratch_shapes=[
            pltpu.VMEM(tokens.shape, BF16),
            pltpu.VMEM(gain.shape, BF16),
            pltpu.VMEM(wq.shape, BF16),
            pltpu.VMEM(wkv.shape, BF16),
            pltpu.VMEM((batches * rows, width), BF16),
            pltpu.VMEM((batches * rows, columns), F32),
            pltpu.VMEM((gx, batches * rows // gx, columns), F32),
            pltpu.SemaphoreType.DMA((2,)),
            pltpu.SemaphoreType.DMA((2, chunks)),
        ],
        compiler_params=params(32),
        name="project",
    )(tokens, gain, wq, wkv)


def stage_kernel(after, cache_hbm, cache, sems):
    del after
    rows = cache.shape[0]
    for r in range(rows):
        pltpu.make_async_copy(cache_hbm.at[r], cache.at[r], sems.at[r]).start()
    for r in range(rows):
        pltpu.make_async_copy(cache_hbm.at[r], cache.at[r], sems.at[r]).wait()


def stage(after, cache):
    return pl.pallas_call(
        stage_kernel,
        out_shape=pltpu.VMEM(cache.shape, BF16),
        in_specs=[ANY, HBM],
        out_specs=VMEM,
        scratch_shapes=[pltpu.SemaphoreType.DMA((cache.shape[0],))],
        compiler_params=params(1),
        name="stage",
    )(after, cache)


def attend_kernel(model_width, parts, angles, *refs):
    received = refs[:parts]
    cache, out, table = refs[parts:]
    rows = cache.shape[0]
    half = HEAD_SIZE // 2
    group = out.shape[1] // HEAD_SIZE
    queries = group * HEAD_SIZE
    sums = received[0][...]
    for k in range(1, parts):
        sums = sums + received[k][...]
    scale = lax.rsqrt(sums[:, queries + 2 * HEAD_SIZE :] / model_width + 1e-05)
    cosine = angles[0]
    sine = angles[1]
    limits = angles[2]

    def rotate(vectors):
        return vectors * cosine + pltpu.roll(vectors, half, 1) * sine

    def column(start):
        return sums[:, start : start + HEAD_SIZE] * scale

    for h in range(group):
        table[pl.ds(h, rows, stride=group), :] = rotate(column(h * HEAD_SIZE))
    rkey = rotate(column(queries))
    value_new = column(queries + HEAD_SIZE)
    inv_root = 1.0 / jnp.sqrt(jnp.float32(HEAD_SIZE))
    pair = 2 if rows % 2 == 0 else 1
    for r in range(0, rows, pair):
        members = range(r, r + pair)
        query = table[r * group : (r + pair) * group, :]
        block = lax.broadcasted_iota(jnp.int32, (pair * group, 1), 0) // group
        left = jnp.concatenate([jnp.where(block == j, query, 0.0) for j in range(pair)], axis=1)
        right = jnp.concatenate([cache[n] for n in members], axis=1)
        scores = (
            lax.dot_general(
                left.astype(BF16), right, (((1,), (1,)), ((), ())), preferred_element_type=F32
            )
            * inv_root
        )

        def spread(vectors):
            return jnp.where(
                block == 0, vectors[r : r + 1, :], vectors[r + pair - 1 : r + pair, :]
            )

        place = lax.broadcasted_iota(jnp.int32, scores.shape, 1)
        place = jnp.where((place & 1) == 0, place, 2 * scores.shape[1]).astype(F32)
        scores = jnp.where(place < spread(limits)[:, :1], scores, -1e30)
        new_score = (
            jnp.sum(query.astype(BF16).astype(F32) * spread(rkey), axis=-1, keepdims=True)
            * inv_root
        )
        top = jnp.maximum(jnp.max(scores, axis=-1, keepdims=True), new_score)
        weights = jnp.exp(scores - top)
        new_weight = jnp.exp(new_score - top)
        total = jnp.sum(weights, axis=-1, keepdims=True) + new_weight
        weights = pltpu.roll(weights, 1, 1).astype(BF16)
        both = jnp.dot(weights, right, preferred_element_type=F32)
        summed = both[:, :HEAD_SIZE]
        for j in range(1, pair):
            summed = jnp.where(block == j, both[:, j * HEAD_SIZE : (j + 1) * HEAD_SIZE], summed)
        summed = summed + new_weight * spread(value_new)
        table[r * group : (r + pair) * group, :] = summed / total
    for h in range(group):
        out[:, h * HEAD_SIZE : (h + 1) * HEAD_SIZE] = table[
            pl.ds(h, rows, stride=group), :
        ].astype(BF16)


def attend(model_width, angles, received, cache, queries):
    rows = cache.shape[0]
    return pl.pallas_call(
        functools.partial(attend_kernel, model_width, len(received)),
        out_shape=jax.ShapeDtypeStruct((rows, queries), BF16),
        in_specs=[VMEM] * (len(received) + 2),
        out_specs=VMEM,
        scratch_shapes=[
            pltpu.VMEM((rows * queries // HEAD_SIZE, HEAD_SIZE), F32),
        ],
        compiler_params=params(4),
        cost_estimate=pl.CostEstimate(flops=10000000000, bytes_accessed=0, transcendentals=0),
        name="attend",
    )(angles, *received, cache)


def output_kernel(gx, batches, *refs):
    received = refs[:gx]
    weights, out, blocks, left = refs[gx:]
    here = received[0].shape[0] // batches
    rows = here * gx
    for k in range(gx):
        blocks[lax.axis_index("gx") ^ k] = received[k][...].astype(F32)
    for place in range(gx):
        for m in range(batches):
            start = m * rows + place * here
            left[start : start + here, :] = blocks[place, m * here : (m + 1) * here, :]
    out[...] = jnp.dot(left[...].astype(BF16), weights[...], preferred_element_type=F32)


def output(received, w_out, batches):
    gx = len(received)
    rows = received[0].shape[0] * gx
    return pl.pallas_call(
        functools.partial(output_kernel, gx, batches),
        out_shape=jax.ShapeDtypeStruct((rows, w_out.shape[1]), F32),
        in_specs=[VMEM] * (gx + 1),
        out_specs=VMEM,
        scratch_shapes=[
            pltpu.VMEM((gx, rows // gx, w_out.shape[0]), F32),
            pltpu.VMEM((rows, w_out.shape[0]), F32),
        ],
        compiler_params=params(4),
        name="output",
    )(*received, w_out)


def rotation(lengths):
    half = HEAD_SIZE // 2
    freq = 500000.0 ** (-2.0 * jnp.arange(half, dtype=F32) / HEAD_SIZE)
    positions = lengths.reshape(-1, 1).astype(F32)
    angle = positions * freq
    cosine = jnp.cos(angle)
    sine = jnp.sin(angle)
    return jnp.stack(
        [
            jnp.concatenate([cosine, cosine], axis=-1),
            jnp.concatenate([-sine, sine], axis=-1),
            jnp.broadcast_to(2.0 * positions, (positions.shape[0], HEAD_SIZE)),
        ]
    )


def add_heads(value, axis, size):
    step = size // 2
    while step > 0:
        if step > 1:
            value = value.astype(BF16)
        other = exchange(value, axis, size, step)
        value = value.astype(F32) + other.astype(F32)
        step //= 2
    return value


def local(gx, gy, tokens, lengths, norm_gain, w_query, key_value_weight, w_out, cache):
    batches, rows, width = tokens.shape
    queries = w_query.shape[1]
    wkv = in_hbm(key_value_weight.reshape(width, -1))
    w_query = in_hbm(w_query)
    pairs = in_hbm(cache.reshape(-1, 2 * cache.shape[2], HEAD_SIZE))
    sent = project(in_hbm(tokens), in_hbm(norm_gain), w_query, wkv, gx)
    pairs = stage(sent[0], pairs)
    received = [sent[0]] + [exchange(sent[k], "gx", gx, k) for k in reversed(range(1, gx))]
    angles = rotation(lengths)
    attended = attend(
        width * gx, angles, received, pairs, queries
    )
    gathered = {k: exchange(attended, "gx", gx, k) for k in reversed(range(1, gx))}
    gathered[0] = attended
    projected = output([gathered[k] for k in range(gx)], w_out, batches)
    summed = add_heads(projected, "gy", gy).reshape(tokens.shape)
    return (tokens.astype(F32) + summed).astype(BF16)


def rotate(vectors, positions):
    half = vectors.shape[-1] // 2
    freq = 500000.0 ** (-2.0 * jnp.arange(half, dtype=F32) / vectors.shape[-1])
    angle = positions[..., None] * freq
    cosine = jnp.cos(angle)
    sine = jnp.sin(angle)
    first = vectors[..., :half]
    second = vectors[..., half:]
    return jnp.concatenate(
        [first * cosine - second * sine, second * cosine + first * sine], axis=-1
    )


def attend_wide(model_width, query_sum, keyval_sum, local_squares, lengths, cache):
    batches, rows_here = lengths.shape
    score_scale = lax.rsqrt(local_squares / model_width + 1e-05)
    heads_kv = keyval_sum.shape[2]
    query_group = query_sum.shape[2] // (heads_kv * HEAD_SIZE)
    query = (
        query_sum.reshape(batches, rows_here, heads_kv, query_group, HEAD_SIZE)
        * score_scale[:, :, None, None, None]
    )
    key_value = keyval_sum * score_scale[:, :, None, None]
    positions = lengths.astype(F32)
    rotated_query = rotate(query, positions[:, :, None, None]).astype(BF16)
    rkey = rotate(key_value[..., :HEAD_SIZE], positions[:, :, None])
    value_new = key_value[..., HEAD_SIZE:]
    inv_root = 1.0 / jnp.sqrt(jnp.float32(HEAD_SIZE))
    keys = cache[:, :, :, :, 0, :]
    values = cache[:, :, :, :, 1, :]
    scores = (
        jnp.einsum("mrkgd,mrskd->mrkgs", rotated_query, keys, preferred_element_type=F32)
        * inv_root
    )
    valid = jnp.arange(cache.shape[2], dtype=jnp.int32)[None, None, :] < lengths[:, :, None]
    scores = jnp.where(valid[:, :, None, None, :], scores, -1e30)
    new_score = jnp.sum(rotated_query.astype(F32) * rkey[:, :, :, None, :], axis=-1) * inv_root
    top = jnp.maximum(jnp.max(scores, axis=-1), new_score)
    weights = jnp.exp(scores - top[..., None])
    new_weight = jnp.exp(new_score - top)
    total = jnp.sum(weights, axis=-1) + new_weight
    summed = jnp.einsum(
        "mrkgs,mrskd->mrkgd", weights.astype(BF16), values, preferred_element_type=F32
    )
    summed = summed + new_weight[..., None] * value_new[:, :, :, None, :]
    return (
        (summed / total[..., None])
        .astype(BF16)
        .reshape(batches, rows_here, heads_kv * query_group * HEAD_SIZE)
    )


def local_wide(gx, tokens, lengths, norm_gain, w_query, key_value_weight, w_out, cache):
    x_full = tokens.astype(F32)
    squares = jnp.sum(x_full * x_full, axis=-1)
    normed = (x_full * norm_gain.astype(F32)).astype(BF16)
    query_part = jnp.einsum("mrd,dc->mrc", normed, w_query, preferred_element_type=F32)
    keyval_part = jnp.einsum("mrd,dkc->mrkc", normed, key_value_weight, preferred_element_type=F32)
    query_sum, keyval_sum, local_squares = (
        lax.psum_scatter(query_part, "gx", scatter_dimension=1, tiled=True),
        lax.psum_scatter(keyval_part, "gx", scatter_dimension=1, tiled=True),
        lax.psum_scatter(squares, "gx", scatter_dimension=1, tiled=True),
    )
    attended = attend_wide(
        tokens.shape[-1] * gx, query_sum, keyval_sum, local_squares, lengths, cache
    )
    projected = jnp.einsum(
        "mrc,cd->mrd",
        lax.all_gather(attended, "gx", axis=1, tiled=True),
        w_out,
        preferred_element_type=F32,
    )
    return (x_full + lax.psum(projected, "gy")).astype(BF16)


def solution(mesh):
    gx, gy = mesh.shape["gx"], mesh.shape["gy"]
    placed = (
        P(None, "groups", "gx"),
        P(None, ("groups", "gx")),
        P("gx"),
        P("gx", "gy"),
        P("gx", "gy", None),
        P("gy", "gx"),
        P(None, ("groups", "gx"), None, "gy", None, None),
    )

    def run(*args):
        kv_heads_here = args[4].shape[1]
        direct = gx <= 8 and gx & (gx - 1) == 0 and gy & (gy - 1) == 0 and kv_heads_here == 1
        if direct:
            return local(gx, gy, *args)
        return local_wide(gx, *args)

    return jax.shard_map(
        run, mesh=mesh, in_specs=placed, out_specs=P(None, "groups", "gx"), check_vma=False
    )
```

```python
import functools

import jax
import jax.numpy as jnp
from jax import lax
from jax.experimental import pallas as pl
from jax.experimental.pallas import tpu as pltpu
from jax.sharding import PartitionSpec as P

HEAD_SIZE = 128
LANES = 128
VMEM = pl.BlockSpec(memory_space=pltpu.VMEM)
ANY = pl.BlockSpec(memory_space=pl.ANY)
HBM = pl.BlockSpec(memory_space=pltpu.HBM)
F32 = jnp.float32
BF16 = jnp.bfloat16


def exchange(value, axis, size, step):
    return lax.ppermute(value, axis, [(i, i ^ step) for i in range(size)])


def in_hbm(value):
    return pltpu.with_memory_space_constraint(value, pltpu.HBM)


def params(mib):
    return pltpu.CompilerParams(vmem_limit_bytes=mib * 2**20)


def project_kernel(chunks, gx, tokens_hbm, gain_hbm, wq_hbm, wkv_hbm, *refs):
    outs = refs[:gx]
    tokens, gain, wq, wkv, normed, sums, staged, small_sems, sems = refs[gx:]
    depth = wq.shape[0] // chunks
    small = [
        pltpu.make_async_copy(tokens_hbm, tokens, small_sems.at[0]),
        pltpu.make_async_copy(gain_hbm, gain, small_sems.at[1]),
    ]
    small[0].start()
    small[1].start()

    def chunk(c):
        part = (pl.ds(c * depth, depth), slice(None))
        return (
            pltpu.make_async_copy(wq_hbm.at[part], wq.at[part], sems.at[0, c]),
            pltpu.make_async_copy(wkv_hbm.at[part], wkv.at[part], sems.at[1, c]),
        )

    @pl.loop(0, chunks)
    def _(c):
        for copy in chunk(c):
            copy.start()

    small[0].wait()
    small[1].wait()
    batches, rows, width = tokens.shape
    total = batches * rows
    queries = wq.shape[1]
    keyvals = wkv.shape[1]
    x_full = tokens[...].astype(F32)
    squares = jnp.sum(x_full * x_full, axis=-1, keepdims=True).reshape(total, 1)
    sums[:, queries + keyvals :] = jnp.broadcast_to(squares, (total, LANES))
    scaled = (x_full * gain[...].astype(F32)).astype(BF16)
    normed[...] = scaled.reshape(total, width)
    for c in range(chunks):
        for copy in chunk(c):
            copy.wait()
        left = normed[:, c * depth : (c + 1) * depth]
        for weights, start, stop in ((wq, 0, queries), (wkv, queries, queries + keyvals)):
            part = jnp.dot(
                left, weights[c * depth : (c + 1) * depth, :], preferred_element_type=F32
            )
            if c == 0:
                sums[:, start:stop] = part
            else:
                sums[:, start:stop] += part
    here = rows // gx
    for place in range(gx):
        for m in range(batches):
            first = m * rows + place * here
            staged[place, m * here : (m + 1) * here, :] = sums[first : first + here, :]
    for k in range(gx):
        outs[k][...] = staged[lax.axis_index("gx") ^ k]


def project(tokens, gain, wq, wkv, gx):
    batches, rows, width = tokens.shape
    columns = wq.shape[1] + wkv.shape[1] + LANES
    chunks = max(1, width // 256)
    return pl.pallas_call(
        functools.partial(project_kernel, chunks, gx),
        out_shape=[jax.ShapeDtypeStruct((batches * rows // gx, columns), F32)] * gx,
        in_specs=[HBM] * 4,
        out_specs=[VMEM] * gx,
        scratch_shapes=[
            pltpu.VMEM(tokens.shape, BF16),
            pltpu.VMEM(gain.shape, BF16),
            pltpu.VMEM(wq.shape, BF16),
            pltpu.VMEM(wkv.shape, BF16),
            pltpu.VMEM((batches * rows, width), BF16),
            pltpu.VMEM((batches * rows, columns), F32),
            pltpu.VMEM((gx, batches * rows // gx, columns), F32),
            pltpu.SemaphoreType.DMA((2,)),
            pltpu.SemaphoreType.DMA((2, chunks)),
        ],
        compiler_params=params(32),
        name="project",
    )(tokens, gain, wq, wkv)


def stage_kernel(after, cache_hbm, keys, values, cache, wide, sems):
    del after
    rows, places, _ = cache.shape
    pair = rows // keys.shape[0]
    copies = [
        pltpu.make_async_copy(cache_hbm.at[r], cache.at[r], sems.at[r]) for r in range(rows)
    ]
    for copy in copies:
        copy.start()
    for r in range(rows):
        copies[r].wait()
        wide[r % 2] = cache[r].astype(F32)
        lanes = slice((r % pair) * HEAD_SIZE, (r % pair + 1) * HEAD_SIZE)
        for start, ref in ((0, keys), (1, values)):
            ref[r // pair, :, lanes] = wide[
                r % 2, pl.ds(start, places // 2, stride=2), :
            ].astype(BF16)


def stage(after, cache):
    rows, places, _ = cache.shape
    pair = 2 if rows % 2 == 0 else 1
    split = pltpu.VMEM((rows // pair, places // 2, pair * HEAD_SIZE), BF16)
    return pl.pallas_call(
        stage_kernel,
        out_shape=[split, split],
        in_specs=[ANY, HBM],
        out_specs=[VMEM, VMEM],
        scratch_shapes=[
            pltpu.VMEM(cache.shape, BF16),
            pltpu.VMEM((2, places, HEAD_SIZE), F32),
            pltpu.SemaphoreType.DMA((rows,)),
        ],
        compiler_params=params(8),
        name="stage",
    )(after, cache)


def attend_kernel(model_width, parts, angles, *refs):
    received = refs[:parts]
    keys, values, out, table = refs[parts:]
    rows = out.shape[0]
    pair = rows // keys.shape[0]
    half = HEAD_SIZE // 2
    group = out.shape[1] // HEAD_SIZE
    queries = group * HEAD_SIZE
    sums = received[0][...]
    for k in range(1, parts):
        sums = sums + received[k][...]
    scale = lax.rsqrt(sums[:, queries + 2 * HEAD_SIZE :] / model_width + 1e-05)
    cosine = angles[0]
    sine = angles[1]
    limits = angles[2]

    def rotate(vectors):
        return vectors * cosine + pltpu.roll(vectors, half, 1) * sine

    def column(start):
        return sums[:, start : start + HEAD_SIZE] * scale

    for h in range(group):
        table[pl.ds(h, rows, stride=group), :] = rotate(column(h * HEAD_SIZE))
    rkey = rotate(column(queries))
    value_new = column(queries + HEAD_SIZE)
    inv_root = 1.0 / jnp.sqrt(jnp.float32(HEAD_SIZE))
    for r in range(0, rows, pair):
        query = table[r * group : (r + pair) * group, :]
        block = lax.broadcasted_iota(jnp.int32, (pair * group, 1), 0) // group
        left = jnp.concatenate([jnp.where(block == j, query, 0.0) for j in range(pair)], axis=1)
        scores = (
            lax.dot_general(
                left.astype(BF16),
                keys[r // pair],
                (((1,), (1,)), ((), ())),
                preferred_element_type=F32,
            )
            * inv_root
        )

        def spread(vectors):
            return jnp.where(
                block == 0, vectors[r : r + 1, :], vectors[r + pair - 1 : r + pair, :]
            )

        place = lax.broadcasted_iota(jnp.int32, scores.shape, 1).astype(F32)
        scores = jnp.where(place < spread(limits)[:, :1], scores, -1e30)
        new_score = (
            jnp.sum(query.astype(BF16).astype(F32) * spread(rkey), axis=-1, keepdims=True)
            * inv_root
        )
        top = jnp.maximum(jnp.max(scores, axis=-1, keepdims=True), new_score)
        weights = jnp.exp(scores - top)
        new_weight = jnp.exp(new_score - top)
        total = jnp.sum(weights, axis=-1, keepdims=True) + new_weight
        both = jnp.dot(weights.astype(BF16), values[r // pair], preferred_element_type=F32)
        summed = both[:, :HEAD_SIZE]
        for j in range(1, pair):
            summed = jnp.where(block == j, both[:, j * HEAD_SIZE : (j + 1) * HEAD_SIZE], summed)
        summed = summed + new_weight * spread(value_new)
        table[r * group : (r + pair) * group, :] = summed / total
    for h in range(group):
        out[:, h * HEAD_SIZE : (h + 1) * HEAD_SIZE] = table[
            pl.ds(h, rows, stride=group), :
        ].astype(BF16)


def attend(model_width, angles, received, keys, values, queries):
    rows = angles.shape[1]
    return pl.pallas_call(
        functools.partial(attend_kernel, model_width, len(received)),
        out_shape=jax.ShapeDtypeStruct((rows, queries), BF16),
        in_specs=[VMEM] * (len(received) + 3),
        out_specs=VMEM,
        scratch_shapes=[
            pltpu.VMEM((rows * queries // HEAD_SIZE, HEAD_SIZE), F32),
        ],
        compiler_params=params(4),
        cost_estimate=pl.CostEstimate(flops=10000000000, bytes_accessed=0, transcendentals=0),
        name="attend",
    )(angles, *received, keys, values)


def output_kernel(gx, batches, *refs):
    received = refs[:gx]
    weights, out, blocks, left = refs[gx:]
    here = received[0].shape[0] // batches
    rows = here * gx
    for k in range(gx):
        blocks[lax.axis_index("gx") ^ k] = received[k][...].astype(F32)
    for place in range(gx):
        for m in range(batches):
            start = m * rows + place * here
            left[start : start + here, :] = blocks[place, m * here : (m + 1) * here, :]
    projected = jnp.dot(left[...].astype(BF16), weights[...], preferred_element_type=F32)
    out[...] = projected.astype(out.dtype)


def output(received, w_out, batches):
    gx = len(received)
    rows = received[0].shape[0] * gx
    return pl.pallas_call(
        functools.partial(output_kernel, gx, batches),
        out_shape=jax.ShapeDtypeStruct((rows, w_out.shape[1]), BF16),
        in_specs=[VMEM] * (gx + 1),
        out_specs=VMEM,
        scratch_shapes=[
            pltpu.VMEM((gx, rows // gx, w_out.shape[0]), F32),
            pltpu.VMEM((rows, w_out.shape[0]), F32),
        ],
        compiler_params=params(4),
        name="output",
    )(*received, w_out)


def rotation(lengths):
    half = HEAD_SIZE // 2
    freq = 500000.0 ** (-2.0 * jnp.arange(half, dtype=F32) / HEAD_SIZE)
    positions = lengths.reshape(-1, 1).astype(F32)
    angle = positions * freq
    cosine = jnp.cos(angle)
    sine = jnp.sin(angle)
    return jnp.stack(
        [
            jnp.concatenate([cosine, cosine], axis=-1),
            jnp.concatenate([-sine, sine], axis=-1),
            jnp.broadcast_to(positions, (positions.shape[0], HEAD_SIZE)),
        ]
    )


def add_heads(value, axis, size):
    step = size // 2
    while step > 0:
        if step > 1:
            value = value.astype(BF16)
        other = exchange(value, axis, size, step)
        value = value.astype(F32) + other.astype(F32)
        step //= 2
    return value


def local(gx, gy, tokens, lengths, norm_gain, w_query, key_value_weight, w_out, cache):
    batches, rows, width = tokens.shape
    queries = w_query.shape[1]
    wkv = in_hbm(key_value_weight.reshape(width, -1))
    w_query = in_hbm(w_query)
    pairs = in_hbm(cache.reshape(-1, 2 * cache.shape[2], HEAD_SIZE))
    sent = project(in_hbm(tokens), in_hbm(norm_gain), w_query, wkv, gx)
    keys, values = stage(sent[0], pairs)
    received = [sent[0]] + [exchange(sent[k], "gx", gx, k) for k in reversed(range(1, gx))]
    angles = rotation(lengths)
    attended = attend(
        width * gx, angles, received, keys, values, queries
    )
    gathered = {k: exchange(attended, "gx", gx, k) for k in reversed(range(1, gx))}
    gathered[0] = attended
    projected = output([gathered[k] for k in range(gx)], w_out, batches)
    summed = add_heads(projected, "gy", gy).reshape(tokens.shape)
    return (tokens.astype(F32) + summed).astype(BF16)


def rotate(vectors, positions):
    half = vectors.shape[-1] // 2
    freq = 500000.0 ** (-2.0 * jnp.arange(half, dtype=F32) / vectors.shape[-1])
    angle = positions[..., None] * freq
    cosine = jnp.cos(angle)
    sine = jnp.sin(angle)
    first = vectors[..., :half]
    second = vectors[..., half:]
    return jnp.concatenate(
        [first * cosine - second * sine, second * cosine + first * sine], axis=-1
    )


def attend_wide(model_width, query_sum, keyval_sum, local_squares, lengths, cache):
    batches, rows_here = lengths.shape
    score_scale = lax.rsqrt(local_squares / model_width + 1e-05)
    heads_kv = keyval_sum.shape[2]
    query_group = query_sum.shape[2] // (heads_kv * HEAD_SIZE)
    query = (
        query_sum.reshape(batches, rows_here, heads_kv, query_group, HEAD_SIZE)
        * score_scale[:, :, None, None, None]
    )
    key_value = keyval_sum * score_scale[:, :, None, None]
    positions = lengths.astype(F32)
    rotated_query = rotate(query, positions[:, :, None, None]).astype(BF16)
    rkey = rotate(key_value[..., :HEAD_SIZE], positions[:, :, None])
    value_new = key_value[..., HEAD_SIZE:]
    inv_root = 1.0 / jnp.sqrt(jnp.float32(HEAD_SIZE))
    keys = cache[:, :, :, :, 0, :]
    values = cache[:, :, :, :, 1, :]
    scores = (
        jnp.einsum("mrkgd,mrskd->mrkgs", rotated_query, keys, preferred_element_type=F32)
        * inv_root
    )
    valid = jnp.arange(cache.shape[2], dtype=jnp.int32)[None, None, :] < lengths[:, :, None]
    scores = jnp.where(valid[:, :, None, None, :], scores, -1e30)
    new_score = jnp.sum(rotated_query.astype(F32) * rkey[:, :, :, None, :], axis=-1) * inv_root
    top = jnp.maximum(jnp.max(scores, axis=-1), new_score)
    weights = jnp.exp(scores - top[..., None])
    new_weight = jnp.exp(new_score - top)
    total = jnp.sum(weights, axis=-1) + new_weight
    summed = jnp.einsum(
        "mrkgs,mrskd->mrkgd", weights.astype(BF16), values, preferred_element_type=F32
    )
    summed = summed + new_weight[..., None] * value_new[:, :, :, None, :]
    return (
        (summed / total[..., None])
        .astype(BF16)
        .reshape(batches, rows_here, heads_kv * query_group * HEAD_SIZE)
    )


def local_wide(gx, tokens, lengths, norm_gain, w_query, key_value_weight, w_out, cache):
    x_full = tokens.astype(F32)
    squares = jnp.sum(x_full * x_full, axis=-1)
    normed = (x_full * norm_gain.astype(F32)).astype(BF16)
    query_part = jnp.einsum("mrd,dc->mrc", normed, w_query, preferred_element_type=F32)
    keyval_part = jnp.einsum("mrd,dkc->mrkc", normed, key_value_weight, preferred_element_type=F32)
    query_sum, keyval_sum, local_squares = (
        lax.psum_scatter(query_part, "gx", scatter_dimension=1, tiled=True),
        lax.psum_scatter(keyval_part, "gx", scatter_dimension=1, tiled=True),
        lax.psum_scatter(squares, "gx", scatter_dimension=1, tiled=True),
    )
    attended = attend_wide(
        tokens.shape[-1] * gx, query_sum, keyval_sum, local_squares, lengths, cache
    )
    projected = jnp.einsum(
        "mrc,cd->mrd",
        lax.all_gather(attended, "gx", axis=1, tiled=True),
        w_out,
        preferred_element_type=F32,
    )
    return (x_full + lax.psum(projected, "gy")).astype(BF16)


def solution(mesh):
    gx, gy = mesh.shape["gx"], mesh.shape["gy"]
    placed = (
        P(None, "groups", "gx"),
        P(None, ("groups", "gx")),
        P("gx"),
        P("gx", "gy"),
        P("gx", "gy", None),
        P("gy", "gx"),
        P(None, ("groups", "gx"), None, "gy", None, None),
    )

    def run(*args):
        kv_heads_here = args[4].shape[1]
        direct = gx <= 8 and gx & (gx - 1) == 0 and gy & (gy - 1) == 0 and kv_heads_here == 1
        if direct:
            return local(gx, gy, *args)
        return local_wide(gx, *args)

    return jax.shard_map(
        run, mesh=mesh, in_specs=placed, out_specs=P(None, "groups", "gx"), check_vma=False
    )
```

```python
import functools

import jax
import jax.numpy as jnp
from jax import lax
from jax.experimental import pallas as pl
from jax.experimental.pallas import tpu as pltpu
from jax.sharding import PartitionSpec as P

HEAD_SIZE = 128
LANES = 128
VMEM = pl.BlockSpec(memory_space=pltpu.VMEM)
ANY = pl.BlockSpec(memory_space=pl.ANY)
HBM = pl.BlockSpec(memory_space=pltpu.HBM)
F32 = jnp.float32
BF16 = jnp.bfloat16


def exchange(value, axis, size, step):
    return lax.ppermute(value, axis, [(i, i ^ step) for i in range(size)])


def in_hbm(value):
    return pltpu.with_memory_space_constraint(value, pltpu.HBM)


def params(mib):
    return pltpu.CompilerParams(vmem_limit_bytes=mib * 2**20)


def project_kernel(depths, gx, tokens_hbm, gain_hbm, wq_hbm, wkv_hbm, *refs):
    outs = refs[:gx]
    tokens, gain, wq, wkv, blocks, left, normed, sums, small_sems, sems = refs[gx:]
    small = [
        pltpu.make_async_copy(tokens_hbm, tokens, small_sems.at[0]),
        pltpu.make_async_copy(gain_hbm, gain, small_sems.at[1]),
    ]
    small[0].start()
    small[1].start()

    def chunk(start, depth, c):
        part = (pl.ds(start, depth), slice(None))
        return (
            pltpu.make_async_copy(wq_hbm.at[part], wq.at[part], sems.at[0, c]),
            pltpu.make_async_copy(wkv_hbm.at[part], wkv.at[part], sems.at[1, c]),
        )

    chunks = []
    start = 0
    for count, depth in depths:
        index = len(chunks)

        @pl.loop(0, count)
        def _(c, start=start, depth=depth, index=index):
            for copy in chunk(start + c * depth, depth, index + c):
                copy.start()

        chunks += [(start + c * depth, depth, index + c) for c in range(count)]
        start += count * depth

    small[0].wait()
    small[1].wait()
    batches, rows, width = tokens.shape
    queries = wq.shape[1]
    keyvals = wkv.shape[1]
    here = rows // gx
    each = batches * here
    x_full = tokens[...].astype(F32)
    squares = jnp.sum(x_full * x_full, axis=-1, keepdims=True)
    scaled = x_full * gain[...].astype(F32)
    for place in range(gx):
        for m in range(batches):
            to = slice(m * here, (m + 1) * here)
            of = slice(place * here, (place + 1) * here)
            blocks[place, to, :width] = scaled[m, of, :]
            blocks[place, to, width:] = jnp.broadcast_to(squares[m, of, :], (here, LANES))
    for k in range(gx):
        left[k * each : (k + 1) * each, :] = blocks[lax.axis_index("gx") ^ k]
    normed[...] = left[:, :width].astype(BF16)
    for k in range(gx):
        outs[k][:, queries + keyvals :] = left[k * each : (k + 1) * each, width:]
    for start, depth, index in chunks:
        for copy in chunk(start, depth, index):
            copy.wait()
        rows_in = slice(start, start + depth)
        for weights, first, last in ((wq, 0, queries), (wkv, queries, queries + keyvals)):
            part = jnp.dot(normed[:, rows_in], weights[rows_in, :], preferred_element_type=F32)
            if start > 0:
                part = part + sums[:, first:last]
            if start + depth < width:
                sums[:, first:last] = part
            else:
                for k in range(gx):
                    outs[k][:, first:last] = part[k * each : (k + 1) * each, :]


def chunk_depths(width):
    if width % 1024 or width == 1024:
        return [(1, width)]
    return [(width // 1024 - 1, 1024), (1, 512), (1, 256), (2, 128)]


def project(tokens, gain, wq, wkv, gx):
    batches, rows, width = tokens.shape
    columns = wq.shape[1] + wkv.shape[1] + LANES
    depths = chunk_depths(width)
    chunks = sum(count for count, _ in depths)
    return pl.pallas_call(
        functools.partial(project_kernel, depths, gx),
        out_shape=[jax.ShapeDtypeStruct((batches * rows // gx, columns), F32)] * gx,
        in_specs=[HBM] * 4,
        out_specs=[VMEM] * gx,
        scratch_shapes=[
            pltpu.VMEM(tokens.shape, BF16),
            pltpu.VMEM(gain.shape, BF16),
            pltpu.VMEM(wq.shape, BF16),
            pltpu.VMEM(wkv.shape, BF16),
            pltpu.VMEM((gx, batches * rows // gx, width + LANES), F32),
            pltpu.VMEM((batches * rows, width + LANES), F32),
            pltpu.VMEM((batches * rows, width), BF16),
            pltpu.VMEM((batches * rows, columns - LANES), F32),
            pltpu.SemaphoreType.DMA((2,)),
            pltpu.SemaphoreType.DMA((2, chunks)),
        ],
        compiler_params=params(32),
        name="project",
    )(tokens, gain, wq, wkv)


def stage_kernel(after, cache_hbm, keys, values, cache, wide, sems):
    del after
    rows, places, _ = cache.shape
    pair = rows // keys.shape[0]
    copies = [
        pltpu.make_async_copy(cache_hbm.at[r], cache.at[r], sems.at[r]) for r in range(rows)
    ]
    for copy in copies:
        copy.start()
    for r in range(rows):
        copies[r].wait()
        wide[r % 2] = cache[r].astype(F32)
        lanes = slice((r % pair) * HEAD_SIZE, (r % pair + 1) * HEAD_SIZE)
        for start, ref in ((0, keys), (1, values)):
            ref[r // pair, :, lanes] = wide[
                r % 2, pl.ds(start, places // 2, stride=2), :
            ].astype(BF16)


def stage(after, cache):
    rows, places, _ = cache.shape
    pair = 2 if rows % 2 == 0 else 1
    split = pltpu.VMEM((rows // pair, places // 2, pair * HEAD_SIZE), BF16)
    return pl.pallas_call(
        stage_kernel,
        out_shape=[split, split],
        in_specs=[ANY, HBM],
        out_specs=[VMEM, VMEM],
        scratch_shapes=[
            pltpu.VMEM(cache.shape, BF16),
            pltpu.VMEM((2, places, HEAD_SIZE), F32),
            pltpu.SemaphoreType.DMA((rows,)),
        ],
        compiler_params=params(8),
        name="stage",
    )(after, cache)


def attend_kernel(model_width, parts, angles, *refs):
    received = refs[:parts]
    keys, values, out, table = refs[parts:]
    rows = out.shape[0]
    pair = rows // keys.shape[0]
    half = HEAD_SIZE // 2
    group = out.shape[1] // HEAD_SIZE
    queries = group * HEAD_SIZE
    sums = received[0][...]
    for k in range(1, parts):
        sums = sums + received[k][...]
    scale = lax.rsqrt(sums[:, queries + 2 * HEAD_SIZE :] / model_width + 1e-05)
    cosine = angles[0]
    sine = angles[1]
    limits = angles[2]

    def rotate(vectors):
        return vectors * cosine + pltpu.roll(vectors, half, 1) * sine

    def column(start):
        return sums[:, start : start + HEAD_SIZE] * scale

    for h in range(group):
        table[pl.ds(h, rows, stride=group), :] = rotate(column(h * HEAD_SIZE))
    rkey = rotate(column(queries))
    value_new = column(queries + HEAD_SIZE)
    inv_root = 1.0 / jnp.sqrt(jnp.float32(HEAD_SIZE))
    for r in range(0, rows, pair):
        query = table[r * group : (r + pair) * group, :]
        block = lax.broadcasted_iota(jnp.int32, (pair * group, 1), 0) // group
        left = jnp.concatenate([jnp.where(block == j, query, 0.0) for j in range(pair)], axis=1)
        scores = (
            lax.dot_general(
                left.astype(BF16),
                keys[r // pair],
                (((1,), (1,)), ((), ())),
                preferred_element_type=F32,
            )
            * inv_root
        )

        def spread(vectors):
            return jnp.where(
                block == 0, vectors[r : r + 1, :], vectors[r + pair - 1 : r + pair, :]
            )

        place = lax.broadcasted_iota(jnp.int32, scores.shape, 1).astype(F32)
        scores = jnp.where(place < spread(limits)[:, :1], scores, -1e30)
        new_score = (
            jnp.sum(query.astype(BF16).astype(F32) * spread(rkey), axis=-1, keepdims=True)
            * inv_root
        )
        top = jnp.maximum(jnp.max(scores, axis=-1, keepdims=True), new_score)
        weights = jnp.exp(scores - top)
        new_weight = jnp.exp(new_score - top)
        total = jnp.sum(weights, axis=-1, keepdims=True) + new_weight
        both = jnp.dot(weights.astype(BF16), values[r // pair], preferred_element_type=F32)
        summed = both[:, :HEAD_SIZE]
        for j in range(1, pair):
            summed = jnp.where(block == j, both[:, j * HEAD_SIZE : (j + 1) * HEAD_SIZE], summed)
        summed = summed + new_weight * spread(value_new)
        table[r * group : (r + pair) * group, :] = summed / total
    for h in range(group):
        out[:, h * HEAD_SIZE : (h + 1) * HEAD_SIZE] = table[
            pl.ds(h, rows, stride=group), :
        ].astype(BF16)


def attend(model_width, angles, received, keys, values, queries):
    rows = angles.shape[1]
    return pl.pallas_call(
        functools.partial(attend_kernel, model_width, len(received)),
        out_shape=jax.ShapeDtypeStruct((rows, queries), BF16),
        in_specs=[VMEM] * (len(received) + 3),
        out_specs=VMEM,
        scratch_shapes=[
            pltpu.VMEM((rows * queries // HEAD_SIZE, HEAD_SIZE), F32),
        ],
        compiler_params=params(4),
        cost_estimate=pl.CostEstimate(flops=10000000000, bytes_accessed=0, transcendentals=0),
        name="attend",
    )(angles, *received, keys, values)


def output_kernel(gx, batches, *refs):
    received = refs[:gx]
    weights, out, blocks, left = refs[gx:]
    here = received[0].shape[0] // batches
    rows = here * gx
    for k in range(gx):
        blocks[lax.axis_index("gx") ^ k] = received[k][...].astype(F32)
    for place in range(gx):
        for m in range(batches):
            start = m * rows + place * here
            left[start : start + here, :] = blocks[place, m * here : (m + 1) * here, :]
    projected = jnp.dot(left[...].astype(BF16), weights[...], preferred_element_type=F32)
    out[...] = projected.astype(out.dtype)


def output(received, w_out, batches):
    gx = len(received)
    rows = received[0].shape[0] * gx
    return pl.pallas_call(
        functools.partial(output_kernel, gx, batches),
        out_shape=jax.ShapeDtypeStruct((rows, w_out.shape[1]), BF16),
        in_specs=[VMEM] * (gx + 1),
        out_specs=VMEM,
        scratch_shapes=[
            pltpu.VMEM((gx, rows // gx, w_out.shape[0]), F32),
            pltpu.VMEM((rows, w_out.shape[0]), F32),
        ],
        compiler_params=params(4),
        name="output",
    )(*received, w_out)


def rotation(lengths):
    half = HEAD_SIZE // 2
    freq = 500000.0 ** (-2.0 * jnp.arange(half, dtype=F32) / HEAD_SIZE)
    positions = lengths.reshape(-1, 1).astype(F32)
    angle = positions * freq
    cosine = jnp.cos(angle)
    sine = jnp.sin(angle)
    return jnp.stack(
        [
            jnp.concatenate([cosine, cosine], axis=-1),
            jnp.concatenate([-sine, sine], axis=-1),
            jnp.broadcast_to(positions, (positions.shape[0], HEAD_SIZE)),
        ]
    )


def add_heads(value, axis, size):
    step = size // 2
    while step > 0:
        value = value.astype(BF16)
        other = exchange(value, axis, size, step)
        value = value.astype(F32) + other.astype(F32)
        step //= 2
    return value


def local(gx, gy, tokens, lengths, norm_gain, w_query, key_value_weight, w_out, cache):
    batches, rows, width = tokens.shape
    queries = w_query.shape[1]
    wkv = in_hbm(key_value_weight.reshape(width, -1))
    w_query = in_hbm(w_query)
    pairs = in_hbm(cache.reshape(-1, 2 * cache.shape[2], HEAD_SIZE))
    sent = project(in_hbm(tokens), in_hbm(norm_gain), w_query, wkv, gx)
    keys, values = stage(sent[0], pairs)
    received = [sent[0]] + [exchange(sent[k], "gx", gx, k) for k in reversed(range(1, gx))]
    angles = rotation(lengths)
    attended = attend(
        width * gx, angles, received, keys, values, queries
    )
    gathered = {k: exchange(attended, "gx", gx, k) for k in reversed(range(1, gx))}
    gathered[0] = attended
    projected = output([gathered[k] for k in range(gx)], w_out, batches)
    summed = add_heads(projected, "gy", gy).reshape(tokens.shape)
    return (tokens.astype(F32) + summed).astype(BF16)


def rotate(vectors, positions):
    half = vectors.shape[-1] // 2
    freq = 500000.0 ** (-2.0 * jnp.arange(half, dtype=F32) / vectors.shape[-1])
    angle = positions[..., None] * freq
    cosine = jnp.cos(angle)
    sine = jnp.sin(angle)
    first = vectors[..., :half]
    second = vectors[..., half:]
    return jnp.concatenate(
        [first * cosine - second * sine, second * cosine + first * sine], axis=-1
    )


def attend_wide(model_width, query_sum, keyval_sum, local_squares, lengths, cache):
    batches, rows_here = lengths.shape
    score_scale = lax.rsqrt(local_squares / model_width + 1e-05)
    heads_kv = keyval_sum.shape[2]
    query_group = query_sum.shape[2] // (heads_kv * HEAD_SIZE)
    query = (
        query_sum.reshape(batches, rows_here, heads_kv, query_group, HEAD_SIZE)
        * score_scale[:, :, None, None, None]
    )
    key_value = keyval_sum * score_scale[:, :, None, None]
    positions = lengths.astype(F32)
    rotated_query = rotate(query, positions[:, :, None, None]).astype(BF16)
    rkey = rotate(key_value[..., :HEAD_SIZE], positions[:, :, None])
    value_new = key_value[..., HEAD_SIZE:]
    inv_root = 1.0 / jnp.sqrt(jnp.float32(HEAD_SIZE))
    keys = cache[:, :, :, :, 0, :]
    values = cache[:, :, :, :, 1, :]
    scores = (
        jnp.einsum("mrkgd,mrskd->mrkgs", rotated_query, keys, preferred_element_type=F32)
        * inv_root
    )
    valid = jnp.arange(cache.shape[2], dtype=jnp.int32)[None, None, :] < lengths[:, :, None]
    scores = jnp.where(valid[:, :, None, None, :], scores, -1e30)
    new_score = jnp.sum(rotated_query.astype(F32) * rkey[:, :, :, None, :], axis=-1) * inv_root
    top = jnp.maximum(jnp.max(scores, axis=-1), new_score)
    weights = jnp.exp(scores - top[..., None])
    new_weight = jnp.exp(new_score - top)
    total = jnp.sum(weights, axis=-1) + new_weight
    summed = jnp.einsum(
        "mrkgs,mrskd->mrkgd", weights.astype(BF16), values, preferred_element_type=F32
    )
    summed = summed + new_weight[..., None] * value_new[:, :, :, None, :]
    return (
        (summed / total[..., None])
        .astype(BF16)
        .reshape(batches, rows_here, heads_kv * query_group * HEAD_SIZE)
    )


def local_wide(gx, tokens, lengths, norm_gain, w_query, key_value_weight, w_out, cache):
    x_full = tokens.astype(F32)
    squares = jnp.sum(x_full * x_full, axis=-1)
    normed = (x_full * norm_gain.astype(F32)).astype(BF16)
    query_part = jnp.einsum("mrd,dc->mrc", normed, w_query, preferred_element_type=F32)
    keyval_part = jnp.einsum("mrd,dkc->mrkc", normed, key_value_weight, preferred_element_type=F32)
    query_sum, keyval_sum, local_squares = (
        lax.psum_scatter(query_part, "gx", scatter_dimension=1, tiled=True),
        lax.psum_scatter(keyval_part, "gx", scatter_dimension=1, tiled=True),
        lax.psum_scatter(squares, "gx", scatter_dimension=1, tiled=True),
    )
    attended = attend_wide(
        tokens.shape[-1] * gx, query_sum, keyval_sum, local_squares, lengths, cache
    )
    projected = jnp.einsum(
        "mrc,cd->mrd",
        lax.all_gather(attended, "gx", axis=1, tiled=True),
        w_out,
        preferred_element_type=F32,
    )
    return (x_full + lax.psum(projected, "gy")).astype(BF16)


def solution(mesh):
    gx, gy = mesh.shape["gx"], mesh.shape["gy"]
    placed = (
        P(None, "groups", "gx"),
        P(None, ("groups", "gx")),
        P("gx"),
        P("gx", "gy"),
        P("gx", "gy", None),
        P("gy", "gx"),
        P(None, ("groups", "gx"), None, "gy", None, None),
    )

    def run(*args):
        kv_heads_here = args[4].shape[1]
        direct = gx <= 8 and gx & (gx - 1) == 0 and gy & (gy - 1) == 0 and kv_heads_here == 1
        if direct:
            return local(gx, gy, *args)
        return local_wide(gx, *args)

    return jax.shard_map(
        run, mesh=mesh, in_specs=placed, out_specs=P(None, "groups", "gx"), check_vma=False
    )
```

```python
import functools

import jax
import jax.numpy as jnp
from jax import lax
from jax.experimental import pallas as pl
from jax.experimental.pallas import tpu as pltpu
from jax.sharding import PartitionSpec as P

HEAD_SIZE = 128
LANES = 128
VMEM = pl.BlockSpec(memory_space=pltpu.VMEM)
ANY = pl.BlockSpec(memory_space=pl.ANY)
HBM = pl.BlockSpec(memory_space=pltpu.HBM)
F32 = jnp.float32
BF16 = jnp.bfloat16
COVER = 10**10


def exchange(value, axis, size, step):
    return lax.ppermute(value, axis, [(i, i ^ step) for i in range(size)])


def in_hbm(value):
    return pltpu.with_memory_space_constraint(value, pltpu.HBM)


def params(mib):
    return pltpu.CompilerParams(vmem_limit_bytes=mib * 2**20)


def project_kernel(depths, gx, tokens_hbm, gain_hbm, wq_hbm, wkv_hbm, *refs):
    outs = refs[:gx]
    tokens, gain, wq, wkv, blocks, left, normed, sums, small_sems, sems = refs[gx:]
    small = [
        pltpu.make_async_copy(tokens_hbm, tokens, small_sems.at[0]),
        pltpu.make_async_copy(gain_hbm, gain, small_sems.at[1]),
    ]
    small[0].start()
    small[1].start()

    def chunk(start, depth, c):
        part = (pl.ds(start, depth), slice(None))
        return (
            pltpu.make_async_copy(wq_hbm.at[part], wq.at[part], sems.at[0, c]),
            pltpu.make_async_copy(wkv_hbm.at[part], wkv.at[part], sems.at[1, c]),
        )

    chunks = []
    start = 0
    for count, depth in depths:
        index = len(chunks)

        @pl.loop(0, count)
        def _(c, start=start, depth=depth, index=index):
            for copy in chunk(start + c * depth, depth, index + c):
                copy.start()

        chunks += [(start + c * depth, depth, index + c) for c in range(count)]
        start += count * depth

    small[0].wait()
    small[1].wait()
    batches, rows, width = tokens.shape
    queries = wq.shape[1]
    keyvals = wkv.shape[1]
    here = rows // gx
    each = batches * here
    x_full = tokens[...].astype(F32)
    squares = jnp.sum(x_full * x_full, axis=-1, keepdims=True)
    scaled = x_full * gain[...].astype(F32)
    for place in range(gx):
        for m in range(batches):
            to = slice(m * here, (m + 1) * here)
            of = slice(place * here, (place + 1) * here)
            blocks[place, to, :width] = scaled[m, of, :]
            blocks[place, to, width:] = jnp.broadcast_to(squares[m, of, :], (here, LANES))
    for k in range(gx):
        left[k * each : (k + 1) * each, :] = blocks[lax.axis_index("gx") ^ k]
    normed[...] = left[:, :width].astype(BF16)
    for k in range(gx):
        outs[k][:, queries + keyvals :] = left[k * each : (k + 1) * each, width:]
    for start, depth, index in chunks:
        for copy in chunk(start, depth, index):
            copy.wait()
        rows_in = slice(start, start + depth)
        for weights, first, last in ((wq, 0, queries), (wkv, queries, queries + keyvals)):
            part = jnp.dot(normed[:, rows_in], weights[rows_in, :], preferred_element_type=F32)
            if start > 0:
                part = part + sums[:, first:last]
            if start + depth < width:
                sums[:, first:last] = part
            else:
                for k in range(gx):
                    outs[k][:, first:last] = part[k * each : (k + 1) * each, :]


def chunk_depths(width):
    if width % 1024 or width == 1024:
        return [(1, width)]
    return [(width // 1024 - 1, 1024), (1, 512), (1, 256), (2, 128)]


def project(tokens, gain, wq, wkv, gx):
    batches, rows, width = tokens.shape
    columns = wq.shape[1] + wkv.shape[1] + LANES
    depths = chunk_depths(width)
    chunks = sum(count for count, _ in depths)
    return pl.pallas_call(
        functools.partial(project_kernel, depths, gx),
        out_shape=[jax.ShapeDtypeStruct((batches * rows // gx, columns), F32)] * gx,
        in_specs=[HBM] * 4,
        out_specs=[VMEM] * gx,
        scratch_shapes=[
            pltpu.VMEM(tokens.shape, BF16),
            pltpu.VMEM(gain.shape, BF16),
            pltpu.VMEM(wq.shape, BF16),
            pltpu.VMEM(wkv.shape, BF16),
            pltpu.VMEM((gx, batches * rows // gx, width + LANES), F32),
            pltpu.VMEM((batches * rows, width + LANES), F32),
            pltpu.VMEM((batches * rows, width), BF16),
            pltpu.VMEM((batches * rows, columns - LANES), F32),
            pltpu.SemaphoreType.DMA((2,)),
            pltpu.SemaphoreType.DMA((2, chunks)),
        ],
        compiler_params=params(32),
        name="project",
    )(tokens, gain, wq, wkv)


def stage_kernel(after, cache_hbm, keys, values, cache, wide, sems):
    del after
    rows, places, _ = cache.shape
    pair = rows // keys.shape[0]
    copies = [
        pltpu.make_async_copy(cache_hbm.at[r], cache.at[r], sems.at[r]) for r in range(rows)
    ]
    for copy in copies:
        copy.start()
    for r in range(rows):
        copies[r].wait()
        wide[r % 2] = cache[r].astype(F32)
        lanes = slice((r % pair) * HEAD_SIZE, (r % pair + 1) * HEAD_SIZE)
        every = [wide[r % 2, pl.ds(k, places // 2, stride=2), :].astype(BF16) for k in range(2)]
        keys[r // pair, lanes, :] = every[0].T
        values[r // pair, :, lanes] = every[1]


def stage(after, cache):
    rows, places, _ = cache.shape
    pair = 2 if rows % 2 == 0 else 1
    split = pltpu.VMEM((rows // pair, places // 2, pair * HEAD_SIZE), BF16)
    turned = pltpu.VMEM((rows // pair, pair * HEAD_SIZE, places // 2), BF16)
    return pl.pallas_call(
        stage_kernel,
        out_shape=[turned, split],
        in_specs=[ANY, HBM],
        out_specs=[VMEM, VMEM],
        scratch_shapes=[
            pltpu.VMEM(cache.shape, BF16),
            pltpu.VMEM((2, places, HEAD_SIZE), F32),
            pltpu.SemaphoreType.DMA((rows,)),
        ],
        compiler_params=params(8),
        name="stage",
    )(after, cache)


def attend_kernel(model_width, parts, angles, *refs):
    received = refs[:parts]
    keys, values, out, table = refs[parts:]
    rows = out.shape[0]
    pair = rows // keys.shape[0]
    half = HEAD_SIZE // 2
    group = out.shape[1] // HEAD_SIZE
    queries = group * HEAD_SIZE
    sums = received[0][...]
    for k in range(1, parts):
        sums = sums + received[k][...]
    scale = lax.rsqrt(sums[:, queries + 2 * HEAD_SIZE :] / model_width + 1e-05)
    cosine = angles[0]
    sine = angles[1]
    limits = angles[2]

    def rotate(vectors):
        return vectors * cosine + pltpu.roll(vectors, half, 1) * sine

    def column(start):
        return sums[:, start : start + HEAD_SIZE] * scale

    for h in range(group):
        table[pl.ds(h, rows, stride=group), :] = rotate(column(h * HEAD_SIZE))
    rkey = rotate(column(queries))
    value_new = column(queries + HEAD_SIZE)
    inv_root = 1.0 / jnp.sqrt(jnp.float32(HEAD_SIZE))
    for r in range(0, rows, pair):
        query = table[r * group : (r + pair) * group, :]
        block = lax.broadcasted_iota(jnp.int32, (pair * group, 1), 0) // group
        left = jnp.concatenate([jnp.where(block == j, query, 0.0) for j in range(pair)], axis=1)
        scores = (
            lax.dot_general(
                left.astype(BF16),
                keys[r // pair],
                (((1,), (0,)), ((), ())),
                preferred_element_type=F32,
            )
            * inv_root
        )

        def spread(vectors):
            return jnp.where(
                block == 0, vectors[r : r + 1, :], vectors[r + pair - 1 : r + pair, :]
            )

        place = lax.broadcasted_iota(jnp.int32, scores.shape, 1).astype(F32)
        scores = jnp.where(place < spread(limits)[:, :1], scores, -1e30)
        new_score = (
            jnp.sum(query.astype(BF16).astype(F32) * spread(rkey), axis=-1, keepdims=True)
            * inv_root
        )
        top = jnp.maximum(jnp.max(scores, axis=-1, keepdims=True), new_score)
        weights = jnp.exp(scores - top)
        new_weight = jnp.exp(new_score - top)
        total = jnp.sum(weights, axis=-1, keepdims=True) + new_weight
        both = jnp.dot(weights.astype(BF16), values[r // pair], preferred_element_type=F32)
        summed = both[:, :HEAD_SIZE]
        for j in range(1, pair):
            summed = jnp.where(block == j, both[:, j * HEAD_SIZE : (j + 1) * HEAD_SIZE], summed)
        summed = summed + new_weight * spread(value_new)
        table[r * group : (r + pair) * group, :] = summed / total
    for h in range(group):
        out[:, h * HEAD_SIZE : (h + 1) * HEAD_SIZE] = table[
            pl.ds(h, rows, stride=group), :
        ].astype(BF16)


def attend(model_width, angles, received, keys, values, queries):
    rows = angles.shape[1]
    return pl.pallas_call(
        functools.partial(attend_kernel, model_width, len(received)),
        out_shape=jax.ShapeDtypeStruct((rows, queries), BF16),
        in_specs=[VMEM] * (len(received) + 3),
        out_specs=VMEM,
        scratch_shapes=[
            pltpu.VMEM((rows * queries // HEAD_SIZE, HEAD_SIZE), F32),
        ],
        compiler_params=params(4),
        cost_estimate=pl.CostEstimate(flops=COVER, bytes_accessed=0, transcendentals=0),
        name="attend",
    )(angles, *received, keys, values)


def output_kernel(gx, batches, *refs):
    received = refs[:gx]
    weights, out, blocks = refs[gx:]
    here = received[0].shape[0] // batches
    for k in range(gx):
        blocks[lax.axis_index("gx") ^ k] = received[k][...].astype(F32)
    left = jnp.concatenate(
        [
            blocks[place, m * here : (m + 1) * here, :]
            for m in range(batches)
            for place in range(gx)
        ],
        axis=0,
    )
    projected = jnp.dot(left.astype(BF16), weights[...], preferred_element_type=F32)
    out[...] = projected.astype(out.dtype)


def output(received, w_out, batches):
    gx = len(received)
    rows = received[0].shape[0] * gx
    return pl.pallas_call(
        functools.partial(output_kernel, gx, batches),
        out_shape=jax.ShapeDtypeStruct((rows, w_out.shape[1]), BF16),
        in_specs=[VMEM] * (gx + 1),
        out_specs=VMEM,
        scratch_shapes=[
            pltpu.VMEM((gx, rows // gx, w_out.shape[0]), F32),
        ],
        compiler_params=params(4),
        name="output",
    )(*received, w_out)


def rotation(lengths):
    half = HEAD_SIZE // 2
    freq = 500000.0 ** (-2.0 * jnp.arange(half, dtype=F32) / HEAD_SIZE)
    positions = lengths.reshape(-1, 1).astype(F32)
    angle = positions * freq
    cosine = jnp.cos(angle)
    sine = jnp.sin(angle)
    return jnp.stack(
        [
            jnp.concatenate([cosine, cosine], axis=-1),
            jnp.concatenate([-sine, sine], axis=-1),
            jnp.broadcast_to(positions, (positions.shape[0], HEAD_SIZE)),
        ]
    )


def add_heads(value, axis, size):
    step = size // 2
    while step > 0:
        value = value.astype(BF16)
        other = exchange(value, axis, size, step)
        value = value.astype(F32) + other.astype(F32)
        step //= 2
    return value


def local(gx, gy, tokens, lengths, norm_gain, w_query, key_value_weight, w_out, cache):
    batches, rows, width = tokens.shape
    queries = w_query.shape[1]
    wkv = in_hbm(key_value_weight.reshape(width, -1))
    w_query = in_hbm(w_query)
    pairs = in_hbm(cache.reshape(-1, 2 * cache.shape[2], HEAD_SIZE))
    sent = project(in_hbm(tokens), in_hbm(norm_gain), w_query, wkv, gx)
    keys, values = stage(sent[0], pairs)
    received = [sent[0]] + [exchange(sent[k], "gx", gx, k) for k in reversed(range(1, gx))]
    angles = rotation(lengths)
    attended = attend(
        width * gx, angles, received, keys, values, queries
    )
    gathered = {k: exchange(attended, "gx", gx, k) for k in reversed(range(1, gx))}
    gathered[0] = attended
    projected = output([gathered[k] for k in range(gx)], w_out, batches)
    summed = add_heads(projected, "gy", gy).reshape(tokens.shape)
    return (tokens.astype(F32) + summed).astype(BF16)


def rotate(vectors, positions):
    half = vectors.shape[-1] // 2
    freq = 500000.0 ** (-2.0 * jnp.arange(half, dtype=F32) / vectors.shape[-1])
    angle = positions[..., None] * freq
    cosine = jnp.cos(angle)
    sine = jnp.sin(angle)
    first = vectors[..., :half]
    second = vectors[..., half:]
    return jnp.concatenate(
        [first * cosine - second * sine, second * cosine + first * sine], axis=-1
    )


def attend_wide(model_width, query_sum, keyval_sum, local_squares, lengths, cache):
    batches, rows_here = lengths.shape
    score_scale = lax.rsqrt(local_squares / model_width + 1e-05)
    heads_kv = keyval_sum.shape[2]
    query_group = query_sum.shape[2] // (heads_kv * HEAD_SIZE)
    query = (
        query_sum.reshape(batches, rows_here, heads_kv, query_group, HEAD_SIZE)
        * score_scale[:, :, None, None, None]
    )
    key_value = keyval_sum * score_scale[:, :, None, None]
    positions = lengths.astype(F32)
    rotated_query = rotate(query, positions[:, :, None, None]).astype(BF16)
    rkey = rotate(key_value[..., :HEAD_SIZE], positions[:, :, None])
    value_new = key_value[..., HEAD_SIZE:]
    inv_root = 1.0 / jnp.sqrt(jnp.float32(HEAD_SIZE))
    keys = cache[:, :, :, :, 0, :]
    values = cache[:, :, :, :, 1, :]
    scores = (
        jnp.einsum("mrkgd,mrskd->mrkgs", rotated_query, keys, preferred_element_type=F32)
        * inv_root
    )
    valid = jnp.arange(cache.shape[2], dtype=jnp.int32)[None, None, :] < lengths[:, :, None]
    scores = jnp.where(valid[:, :, None, None, :], scores, -1e30)
    new_score = jnp.sum(rotated_query.astype(F32) * rkey[:, :, :, None, :], axis=-1) * inv_root
    top = jnp.maximum(jnp.max(scores, axis=-1), new_score)
    weights = jnp.exp(scores - top[..., None])
    new_weight = jnp.exp(new_score - top)
    total = jnp.sum(weights, axis=-1) + new_weight
    summed = jnp.einsum(
        "mrkgs,mrskd->mrkgd", weights.astype(BF16), values, preferred_element_type=F32
    )
    summed = summed + new_weight[..., None] * value_new[:, :, :, None, :]
    return (
        (summed / total[..., None])
        .astype(BF16)
        .reshape(batches, rows_here, heads_kv * query_group * HEAD_SIZE)
    )


def local_wide(gx, tokens, lengths, norm_gain, w_query, key_value_weight, w_out, cache):
    x_full = tokens.astype(F32)
    squares = jnp.sum(x_full * x_full, axis=-1)
    normed = (x_full * norm_gain.astype(F32)).astype(BF16)
    query_part = jnp.einsum("mrd,dc->mrc", normed, w_query, preferred_element_type=F32)
    keyval_part = jnp.einsum("mrd,dkc->mrkc", normed, key_value_weight, preferred_element_type=F32)
    query_sum, keyval_sum, local_squares = (
        lax.psum_scatter(query_part, "gx", scatter_dimension=1, tiled=True),
        lax.psum_scatter(keyval_part, "gx", scatter_dimension=1, tiled=True),
        lax.psum_scatter(squares, "gx", scatter_dimension=1, tiled=True),
    )
    attended = attend_wide(
        tokens.shape[-1] * gx, query_sum, keyval_sum, local_squares, lengths, cache
    )
    projected = jnp.einsum(
        "mrc,cd->mrd",
        lax.all_gather(attended, "gx", axis=1, tiled=True),
        w_out,
        preferred_element_type=F32,
    )
    return (x_full + lax.psum(projected, "gy")).astype(BF16)


def solution(mesh):
    gx, gy = mesh.shape["gx"], mesh.shape["gy"]
    placed = (
        P(None, "groups", "gx"),
        P(None, ("groups", "gx")),
        P("gx"),
        P("gx", "gy"),
        P("gx", "gy", None),
        P("gy", "gx"),
        P(None, ("groups", "gx"), None, "gy", None, None),
    )

    def run(*args):
        kv_heads_here = args[4].shape[1]
        direct = gx <= 8 and gx & (gx - 1) == 0 and gy & (gy - 1) == 0 and kv_heads_here == 1
        if direct:
            return local(gx, gy, *args)
        return local_wide(gx, *args)

    return jax.shard_map(
        run, mesh=mesh, in_specs=placed, out_specs=P(None, "groups", "gx"), check_vma=False
    )
```

```python
import functools

import jax
import jax.numpy as jnp
from jax import lax
from jax.experimental import pallas as pl
from jax.experimental.pallas import tpu as pltpu
from jax.sharding import PartitionSpec as P

HEAD_SIZE = 128
LANES = 128
VMEM = pl.BlockSpec(memory_space=pltpu.VMEM)
ANY = pl.BlockSpec(memory_space=pl.ANY)
HBM = pl.BlockSpec(memory_space=pltpu.HBM)
F32 = jnp.float32
BF16 = jnp.bfloat16
COVER = 10**10


def exchange(value, axis, size, step):
    return lax.ppermute(value, axis, [(i, i ^ step) for i in range(size)])


def in_hbm(value):
    return pltpu.with_memory_space_constraint(value, pltpu.HBM)


def params(mib):
    return pltpu.CompilerParams(vmem_limit_bytes=mib * 2**20)


def project_kernel(depths, gx, tokens_hbm, gain_hbm, wq_hbm, wkv_hbm, *refs):
    outs = refs[:gx]
    tokens, gain, wq, wkv, blocks, left, normed, sums, small_sems, sems = refs[gx:]
    small = [
        pltpu.make_async_copy(tokens_hbm, tokens, small_sems.at[0]),
        pltpu.make_async_copy(gain_hbm, gain, small_sems.at[1]),
    ]
    small[0].start()
    small[1].start()

    def chunk(start, depth, c):
        part = (pl.ds(start, depth), slice(None))
        return (
            pltpu.make_async_copy(wq_hbm.at[part], wq.at[part], sems.at[0, c]),
            pltpu.make_async_copy(wkv_hbm.at[part], wkv.at[part], sems.at[1, c]),
        )

    chunks = []
    start = 0
    for count, depth in depths:
        index = len(chunks)

        @pl.loop(0, count)
        def _(c, start=start, depth=depth, index=index):
            for copy in chunk(start + c * depth, depth, index + c):
                copy.start()

        chunks += [(start + c * depth, depth, index + c) for c in range(count)]
        start += count * depth

    small[0].wait()
    small[1].wait()
    batches, rows, width = tokens.shape
    queries = wq.shape[1]
    keyvals = wkv.shape[1]
    here = rows // gx
    each = batches * here
    x_full = tokens[...].astype(F32)
    squares = jnp.sum(x_full * x_full, axis=-1, keepdims=True)
    scaled = x_full * gain[...].astype(F32)
    for place in range(gx):
        for m in range(batches):
            to = slice(m * here, (m + 1) * here)
            of = slice(place * here, (place + 1) * here)
            blocks[place, to, :width] = scaled[m, of, :]
            blocks[place, to, width:] = jnp.broadcast_to(squares[m, of, :], (here, LANES))
    for k in range(gx):
        left[k * each : (k + 1) * each, :] = blocks[lax.axis_index("gx") ^ k]
    normed[...] = left[:, :width].astype(BF16)
    for k in range(gx):
        outs[k][:, queries + keyvals :] = left[k * each : (k + 1) * each, width:]
    for start, depth, index in chunks:
        for copy in chunk(start, depth, index):
            copy.wait()
        rows_in = slice(start, start + depth)
        for weights, first, last in ((wq, 0, queries), (wkv, queries, queries + keyvals)):
            part = jnp.dot(normed[:, rows_in], weights[rows_in, :], preferred_element_type=F32)
            if start > 0:
                part = part + sums[:, first:last]
            if start + depth < width:
                sums[:, first:last] = part
            else:
                for k in range(gx):
                    outs[k][:, first:last] = part[k * each : (k + 1) * each, :]


def chunk_depths(width):
    if width % 1024 or width == 1024:
        return [(1, width)]
    return [(2, 128), (width // 1024 - 1, 1024), (1, 512), (2, 128)]


def project(tokens, gain, wq, wkv, gx):
    batches, rows, width = tokens.shape
    columns = wq.shape[1] + wkv.shape[1] + LANES
    depths = chunk_depths(width)
    chunks = sum(count for count, _ in depths)
    return pl.pallas_call(
        functools.partial(project_kernel, depths, gx),
        out_shape=[jax.ShapeDtypeStruct((batches * rows // gx, columns), F32)] * gx,
        in_specs=[HBM] * 4,
        out_specs=[VMEM] * gx,
        scratch_shapes=[
            pltpu.VMEM(tokens.shape, BF16),
            pltpu.VMEM(gain.shape, BF16),
            pltpu.VMEM(wq.shape, BF16),
            pltpu.VMEM(wkv.shape, BF16),
            pltpu.VMEM((gx, batches * rows // gx, width + LANES), F32),
            pltpu.VMEM((batches * rows, width + LANES), F32),
            pltpu.VMEM((batches * rows, width), BF16),
            pltpu.VMEM((batches * rows, columns - LANES), F32),
            pltpu.SemaphoreType.DMA((2,)),
            pltpu.SemaphoreType.DMA((2, chunks)),
        ],
        compiler_params=params(32),
        name="project",
    )(tokens, gain, wq, wkv)


def stage_kernel(after, cache_hbm, keys, values, cache, wide, sems):
    del after
    rows, places, _ = cache.shape
    pair = rows // keys.shape[0]
    copies = [
        pltpu.make_async_copy(cache_hbm.at[r], cache.at[r], sems.at[r]) for r in range(rows)
    ]
    for copy in copies:
        copy.start()
    for r in range(rows):
        copies[r].wait()
        wide[r % 2] = cache[r].astype(F32)
        lanes = slice((r % pair) * HEAD_SIZE, (r % pair + 1) * HEAD_SIZE)
        every = [wide[r % 2, pl.ds(k, places // 2, stride=2), :].astype(BF16) for k in range(2)]
        keys[r // pair, lanes, :] = every[0].T
        values[r // pair, :, lanes] = every[1]


def stage(after, cache):
    rows, places, _ = cache.shape
    pair = 2 if rows % 2 == 0 else 1
    split = pltpu.VMEM((rows // pair, places // 2, pair * HEAD_SIZE), BF16)
    turned = pltpu.VMEM((rows // pair, pair * HEAD_SIZE, places // 2), BF16)
    return pl.pallas_call(
        stage_kernel,
        out_shape=[turned, split],
        in_specs=[ANY, HBM],
        out_specs=[VMEM, VMEM],
        scratch_shapes=[
            pltpu.VMEM(cache.shape, BF16),
            pltpu.VMEM((2, places, HEAD_SIZE), F32),
            pltpu.SemaphoreType.DMA((rows,)),
        ],
        compiler_params=params(8),
        name="stage",
    )(after, cache)


def attend_kernel(model_width, parts, angles, *refs):
    received = refs[:parts]
    keys, values, out, table = refs[parts:]
    rows = out.shape[0]
    pair = rows // keys.shape[0]
    half = HEAD_SIZE // 2
    group = out.shape[1] // HEAD_SIZE
    queries = group * HEAD_SIZE
    sums = received[0][...]
    for k in range(1, parts):
        sums = sums + received[k][...]
    scale = lax.rsqrt(sums[:, queries + 2 * HEAD_SIZE :] / model_width + 1e-05)
    cosine = angles[0]
    sine = angles[1]
    limits = angles[2]

    def rotate(vectors):
        return vectors * cosine + pltpu.roll(vectors, half, 1) * sine

    def column(start):
        return sums[:, start : start + HEAD_SIZE] * scale

    for h in range(group):
        table[pl.ds(h, rows, stride=group), :] = rotate(column(h * HEAD_SIZE))
    rkey = rotate(column(queries))
    value_new = column(queries + HEAD_SIZE)
    inv_root = 1.0 / jnp.sqrt(jnp.float32(HEAD_SIZE))
    for r in range(0, rows, pair):
        query = table[r * group : (r + pair) * group, :]
        block = lax.broadcasted_iota(jnp.int32, (pair * group, 1), 0) // group
        left = jnp.concatenate([jnp.where(block == j, query, 0.0) for j in range(pair)], axis=1)
        scores = (
            lax.dot_general(
                left.astype(BF16),
                keys[r // pair],
                (((1,), (0,)), ((), ())),
                preferred_element_type=F32,
            )
            * inv_root
        )

        def spread(vectors):
            return jnp.where(
                block == 0, vectors[r : r + 1, :], vectors[r + pair - 1 : r + pair, :]
            )

        place = lax.broadcasted_iota(jnp.int32, scores.shape, 1).astype(F32)
        scores = jnp.where(place < spread(limits)[:, :1], scores, -1e30)
        new_score = (
            jnp.sum(query.astype(BF16).astype(F32) * spread(rkey), axis=-1, keepdims=True)
            * inv_root
        )
        top = jnp.maximum(jnp.max(scores, axis=-1, keepdims=True), new_score)
        weights = jnp.exp(scores - top)
        new_weight = jnp.exp(new_score - top)
        total = jnp.sum(weights, axis=-1, keepdims=True) + new_weight
        both = jnp.dot(weights.astype(BF16), values[r // pair], preferred_element_type=F32)
        summed = both[:, :HEAD_SIZE]
        for j in range(1, pair):
            summed = jnp.where(block == j, both[:, j * HEAD_SIZE : (j + 1) * HEAD_SIZE], summed)
        summed = summed + new_weight * spread(value_new)
        table[r * group : (r + pair) * group, :] = summed / total
    for h in range(group):
        out[:, h * HEAD_SIZE : (h + 1) * HEAD_SIZE] = table[
            pl.ds(h, rows, stride=group), :
        ].astype(BF16)


def attend(model_width, angles, received, keys, values, queries):
    rows = angles.shape[1]
    return pl.pallas_call(
        functools.partial(attend_kernel, model_width, len(received)),
        out_shape=jax.ShapeDtypeStruct((rows, queries), BF16),
        in_specs=[VMEM] * (len(received) + 3),
        out_specs=VMEM,
        scratch_shapes=[
            pltpu.VMEM((rows * queries // HEAD_SIZE, HEAD_SIZE), F32),
        ],
        compiler_params=params(4),
        cost_estimate=pl.CostEstimate(flops=COVER, bytes_accessed=0, transcendentals=0),
        name="attend",
    )(angles, *received, keys, values)


def output_kernel(gx, batches, *refs):
    received = refs[:gx]
    weights, out, blocks = refs[gx:]
    here = received[0].shape[0] // batches
    for k in range(gx):
        blocks[lax.axis_index("gx") ^ k] = received[k][...].astype(F32)
    left = jnp.concatenate(
        [
            blocks[place, m * here : (m + 1) * here, :]
            for m in range(batches)
            for place in range(gx)
        ],
        axis=0,
    )
    projected = jnp.dot(left.astype(BF16), weights[...], preferred_element_type=F32)
    out[...] = projected.astype(out.dtype)


def output(received, w_out, batches):
    gx = len(received)
    rows = received[0].shape[0] * gx
    return pl.pallas_call(
        functools.partial(output_kernel, gx, batches),
        out_shape=jax.ShapeDtypeStruct((rows, w_out.shape[1]), BF16),
        in_specs=[VMEM] * (gx + 1),
        out_specs=VMEM,
        scratch_shapes=[
            pltpu.VMEM((gx, rows // gx, w_out.shape[0]), F32),
        ],
        compiler_params=params(4),
        name="output",
    )(*received, w_out)


def rotation(lengths):
    half = HEAD_SIZE // 2
    freq = 500000.0 ** (-2.0 * jnp.arange(half, dtype=F32) / HEAD_SIZE)
    positions = lengths.reshape(-1, 1).astype(F32)
    angle = positions * freq
    cosine = jnp.cos(angle)
    sine = jnp.sin(angle)
    return jnp.stack(
        [
            jnp.concatenate([cosine, cosine], axis=-1),
            jnp.concatenate([-sine, sine], axis=-1),
            jnp.broadcast_to(positions, (positions.shape[0], HEAD_SIZE)),
        ]
    )


def add_heads(value, axis, size):
    step = size // 2
    while step > 0:
        value = value.astype(BF16)
        other = exchange(value, axis, size, step)
        value = value.astype(F32) + other.astype(F32)
        step //= 2
    return value


def local(gx, gy, tokens, lengths, norm_gain, w_query, key_value_weight, w_out, cache):
    batches, rows, width = tokens.shape
    queries = w_query.shape[1]
    wkv = in_hbm(key_value_weight.reshape(width, -1))
    w_query = in_hbm(w_query)
    pairs = in_hbm(cache.reshape(-1, 2 * cache.shape[2], HEAD_SIZE))
    sent = project(in_hbm(tokens), in_hbm(norm_gain), w_query, wkv, gx)
    keys, values = stage(sent[0], pairs)
    received = [sent[0]] + [exchange(sent[k], "gx", gx, k) for k in reversed(range(1, gx))]
    angles = rotation(lengths)
    attended = attend(
        width * gx, angles, received, keys, values, queries
    )
    gathered = {k: exchange(attended, "gx", gx, k) for k in reversed(range(1, gx))}
    gathered[0] = attended
    projected = output([gathered[k] for k in range(gx)], w_out, batches)
    summed = add_heads(projected, "gy", gy).reshape(tokens.shape)
    return (tokens.astype(F32) + summed).astype(BF16)


def rotate(vectors, positions):
    half = vectors.shape[-1] // 2
    freq = 500000.0 ** (-2.0 * jnp.arange(half, dtype=F32) / vectors.shape[-1])
    angle = positions[..., None] * freq
    cosine = jnp.cos(angle)
    sine = jnp.sin(angle)
    first = vectors[..., :half]
    second = vectors[..., half:]
    return jnp.concatenate(
        [first * cosine - second * sine, second * cosine + first * sine], axis=-1
    )


def attend_wide(model_width, query_sum, keyval_sum, local_squares, lengths, cache):
    batches, rows_here = lengths.shape
    score_scale = lax.rsqrt(local_squares / model_width + 1e-05)
    heads_kv = keyval_sum.shape[2]
    query_group = query_sum.shape[2] // (heads_kv * HEAD_SIZE)
    query = (
        query_sum.reshape(batches, rows_here, heads_kv, query_group, HEAD_SIZE)
        * score_scale[:, :, None, None, None]
    )
    key_value = keyval_sum * score_scale[:, :, None, None]
    positions = lengths.astype(F32)
    rotated_query = rotate(query, positions[:, :, None, None]).astype(BF16)
    rkey = rotate(key_value[..., :HEAD_SIZE], positions[:, :, None])
    value_new = key_value[..., HEAD_SIZE:]
    inv_root = 1.0 / jnp.sqrt(jnp.float32(HEAD_SIZE))
    keys = cache[:, :, :, :, 0, :]
    values = cache[:, :, :, :, 1, :]
    scores = (
        jnp.einsum("mrkgd,mrskd->mrkgs", rotated_query, keys, preferred_element_type=F32)
        * inv_root
    )
    valid = jnp.arange(cache.shape[2], dtype=jnp.int32)[None, None, :] < lengths[:, :, None]
    scores = jnp.where(valid[:, :, None, None, :], scores, -1e30)
    new_score = jnp.sum(rotated_query.astype(F32) * rkey[:, :, :, None, :], axis=-1) * inv_root
    top = jnp.maximum(jnp.max(scores, axis=-1), new_score)
    weights = jnp.exp(scores - top[..., None])
    new_weight = jnp.exp(new_score - top)
    total = jnp.sum(weights, axis=-1) + new_weight
    summed = jnp.einsum(
        "mrkgs,mrskd->mrkgd", weights.astype(BF16), values, preferred_element_type=F32
    )
    summed = summed + new_weight[..., None] * value_new[:, :, :, None, :]
    return (
        (summed / total[..., None])
        .astype(BF16)
        .reshape(batches, rows_here, heads_kv * query_group * HEAD_SIZE)
    )


def local_wide(gx, tokens, lengths, norm_gain, w_query, key_value_weight, w_out, cache):
    x_full = tokens.astype(F32)
    squares = jnp.sum(x_full * x_full, axis=-1)
    normed = (x_full * norm_gain.astype(F32)).astype(BF16)
    query_part = jnp.einsum("mrd,dc->mrc", normed, w_query, preferred_element_type=F32)
    keyval_part = jnp.einsum("mrd,dkc->mrkc", normed, key_value_weight, preferred_element_type=F32)
    query_sum, keyval_sum, local_squares = (
        lax.psum_scatter(query_part, "gx", scatter_dimension=1, tiled=True),
        lax.psum_scatter(keyval_part, "gx", scatter_dimension=1, tiled=True),
        lax.psum_scatter(squares, "gx", scatter_dimension=1, tiled=True),
    )
    attended = attend_wide(
        tokens.shape[-1] * gx, query_sum, keyval_sum, local_squares, lengths, cache
    )
    projected = jnp.einsum(
        "mrc,cd->mrd",
        lax.all_gather(attended, "gx", axis=1, tiled=True),
        w_out,
        preferred_element_type=F32,
    )
    return (x_full + lax.psum(projected, "gy")).astype(BF16)


def solution(mesh):
    gx, gy = mesh.shape["gx"], mesh.shape["gy"]
    placed = (
        P(None, "groups", "gx"),
        P(None, ("groups", "gx")),
        P("gx"),
        P("gx", "gy"),
        P("gx", "gy", None),
        P("gy", "gx"),
        P(None, ("groups", "gx"), None, "gy", None, None),
    )

    def run(*args):
        kv_heads_here = args[4].shape[1]
        direct = gx <= 8 and gx & (gx - 1) == 0 and gy & (gy - 1) == 0 and kv_heads_here == 1
        if direct:
            return local(gx, gy, *args)
        return local_wide(gx, *args)

    return jax.shard_map(
        run, mesh=mesh, in_specs=placed, out_specs=P(None, "groups", "gx"), check_vma=False
    )
```
